8 devices in a mesh: dp: 2 (over z, y), cp: 4 (over x, core).
Axes of the slice: x: 2, y: 2, z: 1, core: 2. Of those that a mesh axis runs over, the one named last changes fastest.
Arguments:
- x_new: bfloat16 [1024, 3584], P(('dp', 'cp')), parts along dimension 0
- k_cache: bfloat16 [32768, 4, 128], P(('dp', 'cp')), parts along dimension 0
- v_cache: bfloat16 [32768, 4, 128], P(('dp', 'cp')), parts along dimension 0
- valid_len: int32 [8], P(('dp', 'cp')), parts along dimension 0
- w_q: bfloat16 [3584, 3584], replicated
- w_k: bfloat16 [3584, 512], replicated
- w_v: bfloat16 [3584, 512], replicated
- w_o: bfloat16 [3584, 3584], replicated
Outputs:
- output 1: bfloat16 [1024, 3584], P(('dp', 'cp')), parts along dimension 0
- output 2: bfloat16 [1024, 4, 128], P(('dp', 'cp')), parts along dimension 0
- output 3: bfloat16 [1024, 4, 128], P(('dp', 'cp')), parts along dimension 0
There are 2 independent parts. The reference program is written for one: setup_inputs(seed, part) draws one part's arguments, and reference() takes and returns one part's arrays. A program takes and returns all parts, laid end to end along the dimension named above; an argument that names none is the same for every part.
All inputs are finite; a program needn't handle non-finite values.
Results may differ from the reference program's by a relative error of at most 0.0107699.
Values are sent between devices in bfloat16 or wider.
A program may use at most 1 GiB of HBM per device.

```python
import jax
import jax.numpy as jnp
from jax import lax

CP = 4
PIECE = 64
CACHE_DEV = 4096
D_MODEL = 3584
HEADS = 28
KV_HEADS = 4
HEAD = 128
TOKENS = 2 * CP * PIECE
CACHE = CP * CACHE_DEV
GROUP = HEADS // KV_HEADS
TOK_DEV = 2 * PIECE
ROPE_BASE = 500000.0


def draw_lengths(key):
    lens_key, order_key = jax.random.split(key)
    lengths = jax.random.randint(lens_key, (CP,), 1, CACHE_DEV + 1, dtype=jnp.int32)
    slot_order = jax.random.permutation(order_key, CP)
    return lengths.at[slot_order[0]].set(CACHE_DEV).at[slot_order[1]].set(1)


def setup_inputs(seed: int = 0, part: int = 0) -> dict:
    base_key = jax.random.key(seed)
    w_keys = jax.random.split(base_key, 4)
    part_keys = jax.random.split(jax.random.fold_in(base_key, part), 4)
    x_new = jax.random.normal(part_keys[0], (TOKENS, D_MODEL), jnp.float32)
    k_cache = jax.random.normal(part_keys[1], (CACHE, KV_HEADS, HEAD), jnp.float32)
    v_cache = jax.random.normal(part_keys[2], (CACHE, KV_HEADS, HEAD), jnp.float32)
    valid_len = draw_lengths(part_keys[3])
    in_scale = D_MODEL ** -0.5
    out_scale = (HEADS * HEAD) ** -0.5
    w_q = jax.random.normal(w_keys[0], (D_MODEL, HEADS * HEAD), jnp.float32) * in_scale
    w_k = jax.random.normal(w_keys[1], (D_MODEL, KV_HEADS * HEAD), jnp.float32) * in_scale
    w_v = jax.random.normal(w_keys[2], (D_MODEL, KV_HEADS * HEAD), jnp.float32) * in_scale
    w_o = jax.random.normal(w_keys[3], (HEADS * HEAD, D_MODEL), jnp.float32) * out_scale
    return {'x_new': x_new.astype(jnp.bfloat16), 'k_cache': k_cache.astype(jnp.bfloat16), 'v_cache': v_cache.astype(jnp.bfloat16), 'valid_len': valid_len, 'w_q': w_q.astype(jnp.bfloat16), 'w_k': w_k.astype(jnp.bfloat16), 'w_v': w_v.astype(jnp.bfloat16), 'w_o': w_o.astype(jnp.bfloat16)}


def segment_positions():
    dev_ids = jnp.arange(CP)[:, None]
    within = jnp.arange(TOK_DEV)[None, :]
    piece_ids = jnp.where(within < PIECE, dev_ids, 2 * CP - 1 - dev_ids)
    return (piece_ids * PIECE + within % PIECE).reshape(TOKENS)


def rope_apply(values, positions):
    half_dim = HEAD // 2
    inv_freq = jnp.power(ROPE_BASE, -jnp.arange(half_dim, dtype=jnp.float32) * (2.0 / HEAD))
    angles = positions.astype(jnp.float32)[:, None] * inv_freq[None, :]
    cos_a = jnp.cos(angles)[:, None, :]
    sin_a = jnp.sin(angles)[:, None, :]
    first_half = values[..., :half_dim]
    second_half = values[..., half_dim:]
    return jnp.concatenate([first_half * cos_a - second_half * sin_a, second_half * cos_a + first_half * sin_a], axis=-1)


def reference(x_new, k_cache, v_cache, valid_len, w_q, w_k, w_v, w_o):
    seg_pos = segment_positions()
    abs_pos = CACHE + seg_pos
    q_proj = jnp.dot(x_new, w_q, preferred_element_type=jnp.float32).reshape(TOKENS, HEADS, HEAD)
    q_all = rope_apply(q_proj, abs_pos).astype(jnp.bfloat16)
    k_proj = jnp.dot(x_new, w_k, preferred_element_type=jnp.float32).reshape(TOKENS, KV_HEADS, HEAD)
    k_new = rope_apply(k_proj, abs_pos).astype(jnp.bfloat16)
    v_new = jnp.dot(x_new, w_v, preferred_element_type=jnp.float32).astype(jnp.bfloat16).reshape(TOKENS, KV_HEADS, HEAD)
    slot_ok = (jnp.arange(CACHE_DEV)[None, :] < valid_len[:, None]).reshape(CACHE)
    q_heads = q_all.reshape(CP, TOK_DEV, KV_HEADS, GROUP, HEAD).transpose(2, 0, 1, 3, 4)
    k_heads = jnp.concatenate([k_cache, k_new], axis=0).transpose(1, 0, 2)
    v_heads = jnp.concatenate([v_cache, v_new], axis=0).transpose(1, 0, 2)
    pos_blocks = seg_pos.reshape(CP, TOK_DEV)
    score_scale = HEAD ** -0.5

    def head_attend(head_args):
        q_head, k_head, v_head = head_args
        key_f32 = k_head.astype(jnp.float32)
        val_f32 = v_head.astype(jnp.float32)

        def block_attend(block_args):
            q_blk, pos_blk = block_args
            scores = jnp.einsum('ngd,ld->ngl', q_blk.astype(jnp.float32), key_f32) * score_scale
            visible = jnp.concatenate([jnp.broadcast_to(slot_ok[None, :], (TOK_DEV, CACHE)), seg_pos[None, :] <= pos_blk[:, None]], axis=1)
            scores = jnp.where(visible[:, None, :], scores, -jnp.inf)
            row_max = scores.max(axis=-1, keepdims=True)
            weights = jnp.exp(scores - row_max)
            denominator = weights.sum(axis=-1)
            numerator = jnp.einsum('ngl,ld->ngd', weights.astype(jnp.bfloat16).astype(jnp.float32), val_f32)
            return numerator / denominator[..., None]

        return lax.map(block_attend, (q_head, pos_blocks))

    attention = lax.map(head_attend, (q_heads, k_heads, v_heads))
    attention = attention.transpose(1, 2, 0, 3, 4).reshape(TOKENS, HEADS * HEAD).astype(jnp.bfloat16)
    y_out = jnp.dot(attention, w_o, preferred_element_type=jnp.float32).astype(jnp.bfloat16)
    return (y_out, k_new, v_new)
```

```python
import functools
import math

import jax
import jax.numpy as jnp
import numpy as np
from jax import lax
from jax.experimental import pallas as pl
from jax.experimental.pallas import tpu as pltpu
from jax.sharding import PartitionSpec as P

ROPE_BASE = 500000.0
MESH = pl.DeviceIdType.MESH
KEY_TILE = 1024
PREP = 128
HIDE = -3e38


def rope_constants(tok_dev, cp_size, cache_len, head_dim):
    piece = tok_dev // 2
    half = head_dim // 2
    inv_freq = ROPE_BASE ** (-np.arange(half, dtype=np.float64) * 2.0 / head_dim)
    within = np.arange(tok_dev)
    rows = []
    for dev in range(cp_size):
        piece_ids = np.where(within < piece, dev, 2 * cp_size - 1 - dev)
        rows.append(cache_len + piece_ids * piece + within % piece)
    angles = np.concatenate(rows).astype(np.float64)[:, None] * inv_freq[None, :]
    cos, sin = np.cos(angles), np.sin(angles)
    cos_full = np.concatenate([cos, cos], axis=1).astype(np.float32)
    sin_full = np.concatenate([-sin, sin], axis=1).astype(np.float32)
    shape = (cp_size // 2, 2 * tok_dev, head_dim)
    return cos_full.reshape(shape), sin_full.reshape(shape)


def dot_t(lhs, rhs):
    return lax.dot_general(lhs, rhs, (((1,), (1,)), ((), ())), preferred_element_type=jnp.float32)


def kernel(dims, len_ref, x_ref, k_ref, v_ref, wq_ref, wk_ref, wv_ref, wo_ref, cos_ref, sin_ref, y_ref, ko_ref, vo_ref,
           xbuf, raw_k, raw_v, lens, kb, vt, kn, vtn, wbuf, wo1, cosb, sinb, qbuf, ob, pb, oall, ost, kvx,
           loc_sem, wq_sem, pair_s, pair_r, q_s, q_r, p_s, p_r, o_s, o_r):
    heads, head_dim, group, tok, cache, cp_size = dims
    my_heads = heads // 2
    half_cols = my_heads * head_dim
    toks = 2 * tok
    pair = 2 * head_dim
    score_c = math.log2(math.e) / math.sqrt(head_dim)

    me = lax.axis_index('cp')
    core = lax.rem(me, 2)
    chip = lax.div(me, 2)
    mate = me + 1 - 2 * core
    peer = lax.rem(me + 2, cp_size)

    def remote(src, dst, send, recv, dev):
        return pltpu.make_async_remote_copy(src_ref=src, dst_ref=dst, send_sem=send, recv_sem=recv, device_id={'cp': dev}, device_id_type=MESH)

    ld_x = pltpu.make_async_copy(x_ref, xbuf.at[pl.ds(pl.multiple_of(core * tok, tok), tok)], loc_sem.at[0])
    ld_cos = pltpu.make_async_copy(cos_ref.at[chip], cosb, loc_sem.at[1])
    ld_sin = pltpu.make_async_copy(sin_ref.at[chip], sinb, loc_sem.at[2])
    ld_k = pltpu.make_async_copy(k_ref.at[:, core], raw_k.at[0], loc_sem.at[3])
    ld_v = pltpu.make_async_copy(v_ref.at[:, core], raw_v.at[0], loc_sem.at[4])
    n_chunk = my_heads // 2

    def ld_wq(j):
        col = pl.multiple_of(core * half_cols + j * pair, pair)
        return pltpu.make_async_copy(wq_ref.at[:, pl.ds(col, pair)], wbuf.at[:, pl.ds(pl.multiple_of(j * pair, pair), pair)], wq_sem.at[j])

    kv_col = pl.multiple_of(core * pair, pair)
    ld_wk = pltpu.make_async_copy(wk_ref.at[:, pl.ds(kv_col, pair)], wo1.at[:, pl.ds(0, pair)], loc_sem.at[5])
    ld_wv = pltpu.make_async_copy(wv_ref.at[:, pl.ds(kv_col, pair)], wo1.at[:, pl.ds(pair, pair)], loc_sem.at[6])
    ld_wo0 = pltpu.make_async_copy(wo_ref.at[:, pl.ds(0, half_cols)], wbuf, loc_sem.at[7])
    ld_wo1 = pltpu.make_async_copy(wo_ref.at[:, pl.ds(half_cols, half_cols)], wo1, loc_sem.at[8])
    ld_x.start()
    ld_wq(0).start()
    ld_cos.start()
    ld_sin.start()
    lens[0] = jnp.full(lens.shape[1:], len_ref[0], jnp.int32)

    barrier = pltpu.get_barrier_semaphore()
    for other in (mate, peer):
        pl.semaphore_signal(barrier, inc=1, device_id={'cp': other}, device_id_type=MESH)
    pl.semaphore_wait(barrier, 2)

    my_rows = pl.ds(pl.multiple_of(core * tok, tok), tok)
    mate_rows = pl.ds(pl.multiple_of((1 - core) * tok, tok), tok)
    cp_x = remote(x_ref, xbuf.at[my_rows], pair_s.at[0], pair_r.at[0], mate)
    cp_len = remote(lens.at[0], lens.at[1], pair_s.at[1], pair_r.at[1], mate)
    cp_k = remote(k_ref.at[:, 1 - core], raw_k.at[1], pair_s.at[2], pair_r.at[2], mate)
    cp_v = remote(v_ref.at[:, 1 - core], raw_v.at[1], pair_s.at[3], pair_r.at[3], mate)
    cp_x.start()
    for j in range(1, n_chunk):
        ld_wq(j).start()
    cp_len.start()
    cp_k.start()
    cp_v.start()
    ld_wk.start()
    ld_wv.start()
    ld_k.start()
    ld_v.start()

    def rope(vals):
        return vals * cosb[...] + pltpu.roll(vals, head_dim // 2, 1) * sinb[...]

    def cp_q(j):
        src = qbuf.at[pl.ds(2 * j, 2)]
        return remote(src, qbuf.at[pl.ds(my_heads + 2 * j, 2)], q_s.at[j], q_r.at[j], peer)

    ld_x.wait()
    ld_cos.wait()
    ld_sin.wait()
    cp_x.wait_recv()

    def q_step(j, carry):
        ld_wq(j).wait()
        proj = jnp.dot(xbuf[...], wbuf[:, pl.ds(pl.multiple_of(j * pair, pair), pair)], preferred_element_type=jnp.float32)
        qbuf[2 * j] = rope(proj[:, :head_dim]).astype(jnp.bfloat16)
        qbuf[2 * j + 1] = rope(proj[:, head_dim:]).astype(jnp.bfloat16)
        cp_q(j).start()
        return carry

    lax.fori_loop(0, n_chunk, q_step, 0)
    ld_wo0.start()

    ld_wk.wait()
    ld_wv.wait()
    k_proj = jnp.dot(xbuf[...], wo1[:, :pair], preferred_element_type=jnp.float32)
    v_proj = jnp.dot(xbuf[...], wo1[:, pair:2 * pair], preferred_element_type=jnp.float32)
    for h in range(2):
        kn[h] = rope(k_proj[:, h * head_dim:(h + 1) * head_dim]).astype(jnp.bfloat16)
        v_h = v_proj[:, h * head_dim:(h + 1) * head_dim].astype(jnp.bfloat16)
        vtn[h] = v_proj[:, h * head_dim:(h + 1) * head_dim].T.astype(jnp.bfloat16)
        kvx[0, :, h * head_dim:(h + 1) * head_dim] = kn[h]
        kvx[1, :, h * head_dim:(h + 1) * head_dim] = v_h
    ld_wo1.start()
    cp_ko = remote(kvx.at[0, mate_rows], kvx.at[2, pl.ds(0, tok)], pair_s.at[4], pair_r.at[4], mate)
    cp_vo = remote(kvx.at[1, mate_rows], kvx.at[2, pl.ds(tok, tok)], pair_s.at[5], pair_r.at[5], mate)
    cp_ko.start()
    cp_vo.start()

    row = lax.broadcasted_iota(jnp.int32, (2 * PREP, 2 * PREP), 0)
    col = lax.broadcasted_iota(jnp.int32, (2 * PREP, 2 * PREP), 1)
    want = jnp.where(row < PREP, 2 * row, 2 * (row - PREP) + 1)
    pick = jnp.where(col == want, 1.0, 0.0).astype(jnp.bfloat16)
    lane = lax.broadcasted_iota(jnp.int32, (PREP, head_dim), 1)
    slot = lax.broadcasted_iota(jnp.int32, (PREP, head_dim), 0)

    def prep(block):
        def step(i, carry):
            at = pl.multiple_of(i * PREP, PREP)
            to = pl.multiple_of(block * cache + i * PREP, PREP)
            both = jnp.concatenate([raw_k[block, pl.ds(at, PREP)].reshape(2 * PREP, head_dim), raw_v[block, pl.ds(at, PREP)].reshape(2 * PREP, head_dim)], axis=1)
            split = jnp.dot(pick, both, preferred_element_type=jnp.float32)
            hidden = jnp.where((slot + at >= lens[block, 0:1, :]) & (lane == 0), HIDE, 0.0).astype(jnp.bfloat16)
            for h in range(2):
                part = split[h * PREP:(h + 1) * PREP]
                kb[h, pl.ds(to, PREP), :head_dim] = part[:, :head_dim].astype(jnp.bfloat16)
                kb[h, pl.ds(to, PREP), head_dim:] = hidden
                vt[h, :, pl.ds(to, PREP)] = part[:, head_dim:].T.astype(jnp.bfloat16)
            return carry

        lax.fori_loop(0, cache // PREP, step, 0)

    ld_k.wait()
    ld_v.wait()
    prep(0)
    cp_len.wait_recv()
    cp_k.wait_recv()
    cp_v.wait_recv()
    prep(1)

    n_tiles = 2 * cache // KEY_TILE
    first_a = 2
    ones_col = jnp.where(lax.broadcasted_iota(jnp.int32, (toks, head_dim), 1) == 0, 1.0, 0.0).astype(jnp.bfloat16)

    def positions(chip_id, axis):
        within = lax.broadcasted_iota(jnp.int32, (toks, toks), axis)
        dev = 2 * chip_id + jnp.where(within >= tok, 1, 0)
        inner = jnp.where(within >= tok, within - tok, within)
        late = inner >= tok // 2
        piece_id = jnp.where(late, 2 * cp_size - 1 - dev, dev)
        return piece_id * (tok // 2) + jnp.where(late, inner - tok // 2, inner)

    def cp_p(h):
        return remote(ob.at[my_heads + h], pb.at[h], p_s.at[h], p_r.at[h], peer)

    def attend(i, carry):
        is_b = jnp.logical_and(i >= first_a, i < first_a + my_heads)
        idx = jnp.where(i < first_a, i, jnp.where(is_b, my_heads + i - first_a, i - my_heads))
        head = jnp.where(is_b, idx - my_heads, idx)
        kvh = lax.div(head, group)
        q_chip = jnp.where(is_b, 1 - chip, chip)

        @pl.when(jnp.logical_and(is_b, lax.rem(head, 2) == 0))
        def _():
            cp_q(lax.div(head, 2)).wait_recv()

        q = qbuf[idx]
        q_aug = jnp.concatenate([q, ones_col], axis=1)
        top = None
        for t in range(n_tiles + 1):
            if t < n_tiles:
                s = dot_t(kb[kvh, t * KEY_TILE:(t + 1) * KEY_TILE], q_aug)
                vals = vt[kvh, :, t * KEY_TILE:(t + 1) * KEY_TILE]
            else:
                s = dot_t(kn[kvh], q)
                s = jnp.where(positions(chip, 0) <= positions(q_chip, 1), s, -jnp.inf)
                vals = vtn[kvh]
            tile_top = jnp.max(s, axis=0, keepdims=True)
            new_top = tile_top if top is None else jnp.maximum(top, tile_top)
            w = jnp.exp2((s - new_top) * score_c)
            w_sum = jnp.sum(w, axis=0, keepdims=True)
            out = jnp.dot(vals, w.astype(jnp.bfloat16), preferred_element_type=jnp.float32)
            if top is None:
                total, acc = w_sum, out
            else:
                keep = jnp.exp2((top - new_top) * score_c)
                total = total * keep + w_sum
                acc = acc * keep + out
            top = new_top
        ob[idx, :head_dim] = acc
        ob[idx, head_dim:head_dim + 8] = jnp.broadcast_to(top, (8, toks))
        ob[idx, head_dim + 8:head_dim + 16] = jnp.broadcast_to(total, (8, toks))

        @pl.when(is_b)
        def _():
            cp_p(head).start()

        return carry

    lax.fori_loop(0, 2 * my_heads, attend, 0)

    cp_ko.wait()
    cp_vo.wait()
    for out_ref, n in ((ko_ref, 0), (vo_ref, 1)):
        out_ref[:, pl.ds(pl.multiple_of(core * pair, pair), pair)] = kvx[n, my_rows]
        out_ref[:, pl.ds(pl.multiple_of((1 - core) * pair, pair), pair)] = kvx[2, n * tok:(n + 1) * tok]

    def cp_o(h):
        col = pl.multiple_of((core * my_heads + h) * head_dim, head_dim)
        return remote(ost.at[h, mate_rows], oall.at[:, pl.ds(col, head_dim)], o_s.at[h], o_r.at[h], mate)

    def combine(h, carry):
        cp_p(h).wait_recv()
        top_a, top_b = ob[h, head_dim:head_dim + 1], pb[h, head_dim:head_dim + 1]
        top = jnp.maximum(top_a, top_b)
        keep_a = jnp.exp2((top_a - top) * score_c)
        keep_b = jnp.exp2((top_b - top) * score_c)
        total = ob[h, head_dim + 8:head_dim + 9] * keep_a + pb[h, head_dim + 8:head_dim + 9] * keep_b
        out = (ob[h, :head_dim] * keep_a + pb[h, :head_dim] * keep_b) / total
        ost[h] = out.T.astype(jnp.bfloat16)
        cp_o(h).start()
        col = pl.multiple_of((core * my_heads + h) * head_dim, head_dim)
        oall[:, pl.ds(col, head_dim)] = ost[h, my_rows]
        return carry

    lax.fori_loop(0, my_heads, combine, 0)
    ld_wo0.wait()
    ld_wo1.wait()

    def drain(h, carry):
        cp_o(h).wait()
        cp_p(h).wait_send()
        return carry

    lax.fori_loop(0, my_heads, drain, 0)
    for half, weights in ((0, wbuf), (1, wo1)):
        for n in range(half_cols // pair):
            part = jnp.dot(oall[...], weights[:, n * pair:(n + 1) * pair], preferred_element_type=jnp.float32)
            y_ref[:, half * half_cols + n * pair:half * half_cols + (n + 1) * pair] = part.astype(jnp.bfloat16)

    for j in range(n_chunk):
        cp_q(j).wait_send()
    for copy in (cp_x, cp_len, cp_k, cp_v):
        copy.wait_send()


def solution(mesh):
    cp_size = mesh.shape['cp']
    row_spec = P(('dp', 'cp'), None)
    cache_spec = P(('dp', 'cp'), None, None)
    len_spec = P(('dp', 'cp'))
    full_spec = P()

    def device_fn(x_new, k_cache, v_cache, valid_len, w_q, w_k, w_v, w_o):
        tok, width = x_new.shape
        cache, kv_heads, head_dim = k_cache.shape
        heads = w_q.shape[1] // head_dim
        my_heads = heads // 2
        toks = 2 * tok
        half_cols = my_heads * head_dim
        cos, sin = rope_constants(tok, cp_size, cache * cp_size, head_dim)
        dims = (heads, head_dim, heads // kv_heads, tok, cache, cp_size)
        bf16, f32 = jnp.bfloat16, jnp.float32
        k4 = k_cache.reshape(cache, 2, 2, head_dim)
        v4 = v_cache.reshape(cache, 2, 2, head_dim)
        any_spec = pl.BlockSpec(memory_space=pl.ANY)
        vmem_spec = pl.BlockSpec(memory_space=pltpu.VMEM)
        dma = pltpu.SemaphoreType.DMA
        y_out, k_new, v_new = pl.pallas_call(
            functools.partial(kernel, dims),
            out_shape=(
                jax.ShapeDtypeStruct((tok, width), bf16),
                jax.ShapeDtypeStruct((tok, kv_heads * head_dim), bf16),
                jax.ShapeDtypeStruct((tok, kv_heads * head_dim), bf16),
            ),
            in_specs=[pl.BlockSpec(memory_space=pltpu.SMEM)] + [any_spec] * 9,
            out_specs=(vmem_spec,) * 3,
            scratch_shapes=[
                pltpu.VMEM((toks, width), bf16),
                pltpu.VMEM((2, cache, 2, head_dim), bf16),
                pltpu.VMEM((2, cache, 2, head_dim), bf16),
                pltpu.VMEM((2, 8, head_dim), jnp.int32),
                pltpu.VMEM((2, 2 * cache, 2 * head_dim), bf16),
                pltpu.VMEM((2, head_dim, 2 * cache), bf16),
                pltpu.VMEM((2, toks, head_dim), bf16),
                pltpu.VMEM((2, head_dim, toks), bf16),
                pltpu.VMEM((width, half_cols), bf16),
                pltpu.VMEM((width, half_cols), bf16),
                pltpu.VMEM((toks, head_dim), f32),
                pltpu.VMEM((toks, head_dim), f32),
                pltpu.VMEM((heads, toks, head_dim), bf16),
                pltpu.VMEM((heads, head_dim + 16, toks), f32),
                pltpu.VMEM((my_heads, head_dim + 16, toks), f32),
                pltpu.VMEM((tok, heads * head_dim), bf16),
                pltpu.VMEM((my_heads, toks, head_dim), bf16),
                pltpu.VMEM((3, toks, 2 * head_dim), bf16),
                dma((9,)), dma((my_heads // 2,)), dma((6,)), dma((6,)),
                dma((my_heads // 2,)), dma((my_heads // 2,)),
                dma((my_heads,)), dma((my_heads,)), dma((my_heads,)), dma((my_heads,)),
            ],
            compiler_params=pltpu.CompilerParams(collective_id=0, has_side_effects=True, vmem_limit_bytes=67043328),
        )(valid_len, x_new, k4, v4, w_q, w_k, w_v, w_o, jnp.asarray(cos), jnp.asarray(sin))
        shape = (tok, kv_heads, head_dim)
        return y_out, k_new.reshape(shape), v_new.reshape(shape)

    return jax.shard_map(device_fn, mesh=mesh, in_specs=(row_spec, cache_spec, cache_spec, len_spec, full_spec, full_spec, full_spec, full_spec), out_specs=(row_spec, cache_spec, cache_spec), check_vma=False)
```

```python
import functools
import math

import jax
import jax.numpy as jnp
import numpy as np
from jax import lax
from jax.experimental import pallas as pl
from jax.experimental.pallas import tpu as pltpu
from jax.sharding import PartitionSpec as P

ROPE_BASE = 500000.0
MESH = pl.DeviceIdType.MESH
KEY_TILE = 1024
SUB = 1024
PV_SUBS = 1
PREP = 128
PREP_GROUPS = 4
HIDE = -3e38


def rope_constants(tok_dev, cp_size, cache_len, head_dim):
    piece = tok_dev // 2
    half = head_dim // 2
    inv_freq = ROPE_BASE ** (-np.arange(half, dtype=np.float64) * 2.0 / head_dim)
    within = np.arange(tok_dev)
    rows = []
    for dev in range(cp_size):
        piece_ids = np.where(within < piece, dev, 2 * cp_size - 1 - dev)
        rows.append(cache_len + piece_ids * piece + within % piece)
    angles = np.concatenate(rows).astype(np.float64)[:, None] * inv_freq[None, :]
    cos, sin = np.cos(angles), np.sin(angles)
    cos_full = np.concatenate([cos, cos], axis=1).astype(np.float32)
    sin_full = np.concatenate([-sin, sin], axis=1).astype(np.float32)
    shape = (cp_size // 2, 2 * tok_dev, head_dim)
    return cos_full.reshape(shape), sin_full.reshape(shape)


def dot_t(lhs, rhs):
    return lax.dot_general(lhs, rhs, (((1,), (1,)), ((), ())), preferred_element_type=jnp.float32)


def kernel(dims, len_ref, x_ref, k_ref, v_ref, wq_ref, wk_ref, wv_ref, wo_ref, cos_ref, sin_ref, y_ref, ko_ref, vo_ref,
           xbuf, raw_k, raw_v, lens, kb, vt, kn, vtn, wbuf, wo1, cosb, sinb, qbuf, ob, pb, oall, ost, kvx, kvr, ybuf, s_scr, sn_scr, acc,
           loc_sem, wq_sem, pair_s, pair_r, q_s, q_r, p_s, p_r, o_s, o_r):
    heads, head_dim, group, tok, cache, cp_size = dims
    my_heads = heads // 2
    half_cols = my_heads * head_dim
    toks = 2 * tok
    pair = 2 * head_dim
    score_c = math.log2(math.e) / math.sqrt(head_dim)

    me = lax.axis_index('cp')
    core = lax.rem(me, 2)
    chip = lax.div(me, 2)
    mate = me + 1 - 2 * core
    peer = lax.rem(me + 2, cp_size)

    def remote(src, dst, send, recv, dev):
        return pltpu.make_async_remote_copy(src_ref=src, dst_ref=dst, send_sem=send, recv_sem=recv, device_id={'cp': dev}, device_id_type=MESH)

    ld_x = pltpu.make_async_copy(x_ref, xbuf.at[pl.ds(pl.multiple_of(core * tok, tok), tok)], loc_sem.at[0])
    ld_cos = pltpu.make_async_copy(cos_ref.at[chip], cosb, loc_sem.at[1])
    ld_sin = pltpu.make_async_copy(sin_ref.at[chip], sinb, loc_sem.at[2])
    ld_k = pltpu.make_async_copy(k_ref.at[:, core], raw_k.at[0], loc_sem.at[3])
    ld_v = pltpu.make_async_copy(v_ref.at[:, core], raw_v.at[0], loc_sem.at[4])
    n_chunk = my_heads // 2

    def ld_wq(j):
        col = pl.multiple_of(core * half_cols + j * pair, pair)
        return pltpu.make_async_copy(wq_ref.at[:, pl.ds(col, pair)], wbuf.at[:, pl.ds(pl.multiple_of(j * pair, pair), pair)], wq_sem.at[j])

    kv_col = pl.multiple_of(core * pair, pair)
    ld_wk = pltpu.make_async_copy(wk_ref.at[:, pl.ds(kv_col, pair)], wo1.at[:, pl.ds(0, pair)], loc_sem.at[5])
    ld_wv = pltpu.make_async_copy(wv_ref.at[:, pl.ds(kv_col, pair)], wo1.at[:, pl.ds(pair, pair)], loc_sem.at[6])
    ld_wo0 = pltpu.make_async_copy(wo_ref.at[:, pl.ds(0, half_cols)], wbuf, loc_sem.at[7])
    ld_wo1 = pltpu.make_async_copy(wo_ref.at[:, pl.ds(half_cols, half_cols)], wo1, loc_sem.at[8])
    ld_x.start()
    ld_k.start()
    ld_v.start()
    lens[0] = jnp.full(lens.shape[1:], len_ref[0], jnp.int32)

    barrier = pltpu.get_barrier_semaphore()
    for other in (mate, peer):
        pl.semaphore_signal(barrier, inc=1, device_id={'cp': other}, device_id_type=MESH)
    pl.semaphore_wait(barrier, 2)

    my_rows = pl.ds(pl.multiple_of(core * tok, tok), tok)
    mate_rows = pl.ds(pl.multiple_of((1 - core) * tok, tok), tok)
    cp_x = remote(x_ref, xbuf.at[my_rows], pair_s.at[0], pair_r.at[0], mate)
    cp_len = remote(lens.at[0], lens.at[1], pair_s.at[1], pair_r.at[1], mate)
    cp_k = remote(k_ref.at[:, 1 - core], raw_k.at[1], pair_s.at[2], pair_r.at[2], mate)
    cp_v = remote(v_ref.at[:, 1 - core], raw_v.at[1], pair_s.at[3], pair_r.at[3], mate)
    cp_x.start()
    cp_len.start()
    for j in range(2):
        ld_wq(j).start()
    cp_k.start()
    cp_v.start()
    for j in range(2, n_chunk):
        ld_wq(j).start()
    ld_wk.start()
    ld_wv.start()
    ld_cos.start()
    ld_sin.start()

    row = lax.broadcasted_iota(jnp.int32, (2 * PREP, 2 * PREP), 0)
    col = lax.broadcasted_iota(jnp.int32, (2 * PREP, 2 * PREP), 1)
    want = jnp.where(row < PREP, 2 * row, 2 * (row - PREP) + 1)
    pick = jnp.where(col == want, 1.0, 0.0).astype(jnp.bfloat16)
    want_back = jnp.where(col < PREP, 2 * col, 2 * (col - PREP) + 1)
    weave = jnp.where(row == want_back, 1.0, 0.0).astype(jnp.bfloat16)
    lane = lax.broadcasted_iota(jnp.int32, (PREP, head_dim), 1)
    slot = lax.broadcasted_iota(jnp.int32, (PREP, head_dim), 0)

    def prep(block):
        flat_k = raw_k.at[block].reshape(2 * cache, head_dim)
        flat_v = raw_v.at[block].reshape(2 * cache, head_dim)

        def step(i, carry):
            for g in range(PREP_GROUPS):
                at = pl.multiple_of((i * PREP_GROUPS + g) * PREP, PREP)
                to = pl.multiple_of(block * cache + at, PREP)
                both = jnp.concatenate([flat_k[pl.ds(2 * at, 2 * PREP)], flat_v[pl.ds(2 * at, 2 * PREP)]], axis=1)
                split = jnp.dot(pick, both, preferred_element_type=jnp.float32).astype(jnp.bfloat16)
                hidden = jnp.where((slot + at >= lens[block, 0:1, :]) & (lane == 0), HIDE, 0.0).astype(jnp.bfloat16)
                for h in range(2):
                    part = split[h * PREP:(h + 1) * PREP]
                    kb[h, pl.ds(to, PREP), :head_dim] = part[:, :head_dim]
                    kb[h, pl.ds(to, PREP), head_dim:] = hidden
                    vt[h, :, pl.ds(to, PREP)] = part[:, head_dim:].T
            return carry

        lax.fori_loop(0, cache // PREP // PREP_GROUPS, step, 0)

    ld_k.wait()
    ld_v.wait()
    prep(0)

    def rope(vals):
        return vals * cosb[...] + pltpu.roll(vals, head_dim // 2, 1) * sinb[...]

    def cp_q(j):
        src = qbuf.at[pl.ds(2 * j, 2)]
        return remote(src, qbuf.at[pl.ds(my_heads + 2 * j, 2)], q_s.at[j], q_r.at[j], peer)

    ld_x.wait()
    ld_cos.wait()
    ld_sin.wait()
    cp_x.wait_recv()

    chunks = [(2 * j, min(2, n_chunk - 2 * j)) for j in range((n_chunk + 1) // 2)]
    for step in range(len(chunks) + 2):
        if step < len(chunks):
            first, count = chunks[step]
            for j in range(first, first + count):
                ld_wq(j).wait()
            proj = jnp.dot(xbuf[...], wbuf[:, first * pair:(first + count) * pair], preferred_element_type=jnp.float32)
        elif step == len(chunks):
            ld_wk.wait()
            ld_wv.wait()
            proj = jnp.dot(xbuf[...], wo1[:, :2 * pair], preferred_element_type=jnp.float32)
        if step >= 1 and step - 1 < len(chunks):
            first, count = chunks[step - 1]
            for j in range(first, first + count):
                for h in range(2):
                    part = s_scr[(step - 1) % 2, (j - first) * toks:(j - first + 1) * toks, h * head_dim:(h + 1) * head_dim]
                    qbuf[2 * j + h] = rope(part).T.astype(jnp.bfloat16)
                cp_q(j).start()
        if step <= len(chunks):
            for n in range(proj.shape[1] // pair):
                s_scr[step % 2, n * toks:(n + 1) * toks] = proj[:, n * pair:(n + 1) * pair]
    ld_wo0.start()
    ld_wo1.start()
    done = len(chunks) % 2
    k_heads = [rope(s_scr[done, :toks, h * head_dim:(h + 1) * head_dim]).astype(jnp.bfloat16) for h in range(2)]
    v_heads = [s_scr[done, toks:2 * toks, h * head_dim:(h + 1) * head_dim].astype(jnp.bfloat16) for h in range(2)]
    for h in range(2):
        kn[h] = k_heads[h]
        vtn[h] = v_heads[h].T
    for part in range(2):
        rows = slice(part * tok, (part + 1) * tok)
        both = jnp.concatenate([jnp.concatenate([k_heads[h][rows], v_heads[h][rows]], axis=1) for h in range(2)], axis=0)
        mixed = jnp.dot(weave, both, preferred_element_type=jnp.float32).astype(jnp.bfloat16)
        for n in range(2):
            kvx[n, rows] = mixed[:, n * head_dim:(n + 1) * head_dim].reshape(tok, 2, head_dim)
    cp_ko = remote(kvx.at[0, mate_rows], kvr.at[0], pair_s.at[4], pair_r.at[4], mate)
    cp_vo = remote(kvx.at[1, mate_rows], kvr.at[1], pair_s.at[5], pair_r.at[5], mate)
    cp_ko.start()
    cp_vo.start()
    outs = [pltpu.make_async_copy(kvx.at[n, my_rows], out_ref.at[:, core], loc_sem.at[9 + n]) for n, out_ref in ((0, ko_ref), (1, vo_ref))]
    for out in outs:
        out.start()

    cp_len.wait_recv()
    cp_k.wait_recv()
    cp_v.wait_recv()
    prep(1)

    n_tiles = 2 * cache // KEY_TILE
    n_sub = KEY_TILE // SUB
    first_a = 2
    new_at = 3
    ones_row = jnp.where(lax.broadcasted_iota(jnp.int32, (head_dim, toks), 0) == 0, 1.0, 0.0).astype(jnp.bfloat16)

    def positions(chip_id, axis):
        within = lax.broadcasted_iota(jnp.int32, (toks, toks), axis)
        dev = 2 * chip_id + jnp.where(within >= tok, 1, 0)
        inner = jnp.where(within >= tok, within - tok, within)
        late = inner >= tok // 2
        piece_id = jnp.where(late, 2 * cp_size - 1 - dev, dev)
        return piece_id * (tok // 2) + jnp.where(late, inner - tok // 2, inner)

    def cp_p(h):
        return remote(ob.at[my_heads + h], pb.at[h], p_s.at[h], p_r.at[h], peer)

    def place(i):
        is_b = jnp.logical_and(i >= first_a, i < first_a + my_heads)
        idx = jnp.where(i < first_a, i, jnp.where(is_b, my_heads + i - first_a, i - my_heads))
        return is_b, idx, jnp.where(is_b, idx - my_heads, idx)

    def peak(s):
        return jnp.max(s.reshape(s.shape[0] // 8, 8, toks), axis=0)

    def scores(kvh, q_aug, t, r):
        s = jnp.dot(kb[kvh, t * KEY_TILE + r * SUB:t * KEY_TILE + (r + 1) * SUB], q_aug, preferred_element_type=jnp.float32)
        s_scr[t % 2, r * SUB:(r + 1) * SUB] = s
        return peak(s)

    def with_ones(q):
        return jnp.concatenate([q, ones_row], axis=0)

    def attend(i, tops):
        is_b, idx, head = place(i)
        kvh = lax.div(head, group)
        q_chip = jnp.where(is_b, 1 - chip, chip)
        after = jnp.minimum(i + 1, 2 * my_heads - 1)
        next_b, next_idx, next_head = place(after)
        next_kvh = lax.div(next_head, group)

        @pl.when(jnp.logical_and(jnp.logical_and(next_b, after > i), lax.rem(next_head, 2) == 0))
        def _():
            cp_q(lax.div(next_head, 2)).wait_recv()

        q_aug = with_ones(qbuf[idx])
        next_q = with_ones(qbuf[next_idx])
        tops = list(tops)
        top = None
        total = None
        for t in range(n_tiles):
            here = tops[t]
            if t == new_at:
                here = jnp.maximum(here, seg_tops)
            tile_top = jnp.max(here, axis=0, keepdims=True)
            new_top = tile_top if top is None else jnp.maximum(top, tile_top)
            keep = None if top is None else jnp.exp2((top - new_top) * score_c)
            top = new_top
            new_tops = None
            w_sum = None
            halves = []
            for r in range(n_sub):
                w = jnp.exp2((s_scr[t % 2, r * SUB:(r + 1) * SUB] - top) * score_c)
                if t + 2 < n_tiles:
                    sub_tops = scores(kvh, q_aug, t + 2, r)
                else:
                    sub_tops = scores(next_kvh, next_q, t + 2 - n_tiles, r)
                new_tops = sub_tops if new_tops is None else jnp.maximum(new_tops, sub_tops)
                part = jnp.sum(w.reshape(SUB // 8, 8, toks), axis=0)
                w_sum = part if w_sum is None else w_sum + part
                halves.append(w.astype(jnp.bfloat16))
                if len(halves) == PV_SUBS:
                    at = t * KEY_TILE + (r + 1 - PV_SUBS) * SUB
                    wide = halves[0] if PV_SUBS == 1 else jnp.concatenate(halves, axis=0)
                    halves = []
                    out = jnp.dot(vt[kvh, :, at:at + PV_SUBS * SUB], wide, preferred_element_type=jnp.float32)
                    if r + 1 > PV_SUBS:
                        acc[...] += out
                    elif keep is None:
                        acc[...] = out
                    else:
                        acc[...] = acc[...] * keep + out
            if t == new_at - 2:
                s = jnp.dot(kn[kvh], qbuf[idx], preferred_element_type=jnp.float32)
                s = jnp.where(positions(chip, 0) <= positions(q_chip, 1), s, -jnp.inf)
                sn_scr[...] = s
                seg_tops = peak(s)
            if t == new_at:
                w = jnp.exp2((sn_scr[...] - top) * score_c)
                w_sum = w_sum + jnp.sum(w.reshape(toks // 8, 8, toks), axis=0)
                acc[...] += jnp.dot(vtn[kvh], w.astype(jnp.bfloat16), preferred_element_type=jnp.float32)
            total = w_sum if keep is None else total * keep + w_sum
            tops.append(new_tops)
        ob[idx, :head_dim] = acc[...]
        ob[idx, head_dim:head_dim + 8] = jnp.broadcast_to(top, (8, toks))
        ob[idx, head_dim + 8:head_dim + 16] = jnp.broadcast_to(jnp.sum(total, axis=0, keepdims=True), (8, toks))

        @pl.when(is_b)
        def _():
            cp_p(head).start()

        return tops[n_tiles], tops[n_tiles + 1]

    first_q = with_ones(qbuf[0])
    start_tops = []
    for t in range(2):
        tops = scores(0, first_q, t, 0)
        for r in range(1, n_sub):
            tops = jnp.maximum(tops, scores(0, first_q, t, r))
        start_tops.append(tops)
    lax.fori_loop(0, 2 * my_heads, attend, tuple(start_tops))

    cp_ko.wait()
    cp_vo.wait()
    more = [pltpu.make_async_copy(kvr.at[n], out_ref.at[:, 1 - core], loc_sem.at[11 + n]) for n, out_ref in ((0, ko_ref), (1, vo_ref))]
    for out in more:
        out.start()

    def cp_o(h):
        col = pl.multiple_of((core * my_heads + h) * head_dim, head_dim)
        return remote(ost.at[h, mate_rows], oall.at[:, pl.ds(col, head_dim)], o_s.at[h], o_r.at[h], mate)

    def combine(h, carry):
        cp_p(h).wait_recv()
        top_a, top_b = ob[h, head_dim:head_dim + 1], pb[h, head_dim:head_dim + 1]
        top = jnp.maximum(top_a, top_b)
        keep_a = jnp.exp2((top_a - top) * score_c)
        keep_b = jnp.exp2((top_b - top) * score_c)
        total = ob[h, head_dim + 8:head_dim + 9] * keep_a + pb[h, head_dim + 8:head_dim + 9] * keep_b
        out = (ob[h, :head_dim] * keep_a + pb[h, :head_dim] * keep_b) / total
        ost[h] = out.T.astype(jnp.bfloat16)
        cp_o(h).start()
        col = pl.multiple_of((core * my_heads + h) * head_dim, head_dim)
        oall[:, pl.ds(col, head_dim)] = ost[h, my_rows]
        return carry

    lax.fori_loop(0, my_heads, combine, 0)
    ld_wo0.wait()
    ld_wo1.wait()

    def drain(h, carry):
        cp_o(h).wait()
        cp_p(h).wait_send()
        return carry

    lax.fori_loop(0, my_heads, drain, 0)
    y_copies = []
    for half, weights in ((0, wbuf), (1, wo1)):
        for n in range(half_cols // pair):
            cols = slice(half * half_cols + n * pair, half * half_cols + (n + 1) * pair)
            part = jnp.dot(oall[...], weights[:, n * pair:(n + 1) * pair], preferred_element_type=jnp.float32)
            ybuf[:, cols] = part.astype(jnp.bfloat16)
        cols = pl.ds(half * half_cols, half_cols)
        y_copies.append(pltpu.make_async_copy(ybuf.at[:, cols], y_ref.at[:, cols], loc_sem.at[13 + half]))
        y_copies[-1].start()
    for out in y_copies + outs + more:
        out.wait()
    for j in range(n_chunk):
        cp_q(j).wait_send()
    for copy in (cp_x, cp_len, cp_k, cp_v):
        copy.wait_send()


def solution(mesh):
    cp_size = mesh.shape['cp']
    row_spec = P(('dp', 'cp'), None)
    cache_spec = P(('dp', 'cp'), None, None)
    len_spec = P(('dp', 'cp'))
    full_spec = P()

    def device_fn(x_new, k_cache, v_cache, valid_len, w_q, w_k, w_v, w_o):
        tok, width = x_new.shape
        cache, kv_heads, head_dim = k_cache.shape
        heads = w_q.shape[1] // head_dim
        my_heads = heads // 2
        toks = 2 * tok
        half_cols = my_heads * head_dim
        cos, sin = rope_constants(tok, cp_size, cache * cp_size, head_dim)
        dims = (heads, head_dim, heads // kv_heads, tok, cache, cp_size)
        bf16, f32 = jnp.bfloat16, jnp.float32
        k4 = k_cache.reshape(cache, 2, 2, head_dim)
        v4 = v_cache.reshape(cache, 2, 2, head_dim)
        any_spec = pl.BlockSpec(memory_space=pl.ANY)
        dma = pltpu.SemaphoreType.DMA
        y_out, k_new, v_new = pl.pallas_call(
            functools.partial(kernel, dims),
            out_shape=(
                jax.ShapeDtypeStruct((tok, width), bf16),
                jax.ShapeDtypeStruct((tok, kv_heads // 2, 2, head_dim), bf16),
                jax.ShapeDtypeStruct((tok, kv_heads // 2, 2, head_dim), bf16),
            ),
            in_specs=[pl.BlockSpec(memory_space=pltpu.SMEM)] + [any_spec] * 9,
            out_specs=(any_spec,) * 3,
            scratch_shapes=[
                pltpu.VMEM((toks, width), bf16),
                pltpu.VMEM((2, cache, 2, head_dim), bf16),
                pltpu.VMEM((2, cache, 2, head_dim), bf16),
                pltpu.VMEM((2, 8, head_dim), jnp.int32),
                pltpu.VMEM((2, 2 * cache, 2 * head_dim), bf16),
                pltpu.VMEM((2, head_dim, 2 * cache), bf16),
                pltpu.VMEM((2, toks, head_dim), bf16),
                pltpu.VMEM((2, head_dim, toks), bf16),
                pltpu.VMEM((width, half_cols), bf16),
                pltpu.VMEM((width, half_cols), bf16),
                pltpu.VMEM((toks, head_dim), f32),
                pltpu.VMEM((toks, head_dim), f32),
                pltpu.VMEM((heads, head_dim, toks), bf16),
                pltpu.VMEM((heads, head_dim + 16, toks), f32),
                pltpu.VMEM((my_heads, head_dim + 16, toks), f32),
                pltpu.VMEM((tok, heads * head_dim), bf16),
                pltpu.VMEM((my_heads, toks, head_dim), bf16),
                pltpu.VMEM((2, toks, 2, head_dim), bf16),
                pltpu.VMEM((2, tok, 2, head_dim), bf16),
                pltpu.VMEM((tok, width), bf16),
                pltpu.VMEM((2, KEY_TILE, toks), f32),
                pltpu.VMEM((toks, toks), f32),
                pltpu.VMEM((head_dim, toks), f32),
                dma((15,)), dma((my_heads // 2,)), dma((6,)), dma((6,)),
                dma((my_heads // 2,)), dma((my_heads // 2,)),
                dma((my_heads,)), dma((my_heads,)), dma((my_heads,)), dma((my_heads,)),
            ],
            compiler_params=pltpu.CompilerParams(collective_id=0, has_side_effects=True, vmem_limit_bytes=67043328),
        )(valid_len, x_new, k4, v4, w_q, w_k, w_v, w_o, jnp.asarray(cos), jnp.asarray(sin))
        shape = (tok, kv_heads, head_dim)
        return y_out, k_new.reshape(shape), v_new.reshape(shape)

    return jax.shard_map(device_fn, mesh=mesh, in_specs=(row_spec, cache_spec, cache_spec, len_spec, full_spec, full_spec, full_spec, full_spec), out_specs=(row_spec, cache_spec, cache_spec), check_vma=False)
```

```python
import functools
import math

import jax
import jax.numpy as jnp
import numpy as np
from jax import lax
from jax.experimental import pallas as pl
from jax.experimental.pallas import tpu as pltpu
from jax.sharding import PartitionSpec as P

ROPE_BASE = 500000.0
MESH = pl.DeviceIdType.MESH
KEY_TILE = 1024
SUB = 1024
PV_SUBS = 1
PREP = 128
PREP_GROUPS = 4
HIDE = -3e38


def rope_constants(tok_dev, cp_size, cache_len, head_dim):
    piece = tok_dev // 2
    half = head_dim // 2
    inv_freq = ROPE_BASE ** (-np.arange(half, dtype=np.float64) * 2.0 / head_dim)
    within = np.arange(tok_dev)
    rows = []
    for dev in range(cp_size):
        piece_ids = np.where(within < piece, dev, 2 * cp_size - 1 - dev)
        rows.append(cache_len + piece_ids * piece + within % piece)
    angles = np.concatenate(rows).astype(np.float64)[:, None] * inv_freq[None, :]
    cos, sin = np.cos(angles), np.sin(angles)
    cos_full = np.concatenate([cos, cos], axis=1).astype(np.float32)
    sin_full = np.concatenate([-sin, sin], axis=1).astype(np.float32)
    shape = (cp_size // 2, 2 * tok_dev, head_dim)
    return cos_full.reshape(shape), sin_full.reshape(shape)


def dot_t(lhs, rhs):
    return lax.dot_general(lhs, rhs, (((1,), (1,)), ((), ())), preferred_element_type=jnp.float32)


def kernel(dims, len_ref, x_ref, k_ref, v_ref, wq_ref, wk_ref, wv_ref, wo_ref, cos_ref, sin_ref, y_ref, ko_ref, vo_ref,
           xbuf, raw_k, raw_v, lens, kb, vt, kn, vtn, wbuf, wo1, cosb, sinb, qbuf, ob, pb, oall, ost, kvx, kvr, ybuf, s_scr, sn_scr, acc,
           loc_sem, wq_sem, pair_s, pair_r, q_s, q_r, p_s, p_r, o_s, o_r):
    heads, head_dim, group, tok, cache, cp_size = dims
    my_heads = heads // 2
    half_cols = my_heads * head_dim
    toks = 2 * tok
    pair = 2 * head_dim
    score_c = math.log2(math.e) / math.sqrt(head_dim)

    me = lax.axis_index('cp')
    core = lax.rem(me, 2)
    chip = lax.div(me, 2)
    mate = me + 1 - 2 * core
    peer = lax.rem(me + 2, cp_size)

    def remote(src, dst, send, recv, dev):
        return pltpu.make_async_remote_copy(src_ref=src, dst_ref=dst, send_sem=send, recv_sem=recv, device_id={'cp': dev}, device_id_type=MESH)

    ld_x = pltpu.make_async_copy(x_ref, xbuf.at[pl.ds(pl.multiple_of(core * tok, tok), tok)], loc_sem.at[0])
    ld_cos = pltpu.make_async_copy(cos_ref.at[chip], cosb, loc_sem.at[1])
    ld_sin = pltpu.make_async_copy(sin_ref.at[chip], sinb, loc_sem.at[2])
    ld_k = pltpu.make_async_copy(k_ref.at[:, core], raw_k.at[0], loc_sem.at[3])
    ld_v = pltpu.make_async_copy(v_ref.at[:, core], raw_v.at[0], loc_sem.at[4])
    n_chunk = my_heads // 2

    def ld_wq(j, sem=None):
        sem = j if sem is None else sem
        col = pl.multiple_of(core * half_cols + j * pair, pair)
        return pltpu.make_async_copy(wq_ref.at[:, pl.ds(col, pair)], wbuf.at[:, pl.ds(pl.multiple_of(j * pair, pair), pair)], wq_sem.at[sem])

    kv_col = pl.multiple_of(core * pair, pair)
    ld_wk = pltpu.make_async_copy(wk_ref.at[:, pl.ds(kv_col, pair)], wbuf.at[:, pl.ds(half_cols, pair)], wq_sem.at[n_chunk])
    ld_wv = pltpu.make_async_copy(wv_ref.at[:, pl.ds(kv_col, pair)], wbuf.at[:, pl.ds(half_cols + pair, pair)], wq_sem.at[n_chunk + 1])
    wide = wbuf.shape[1]
    rest = wo1.shape[1]
    ld_wo0 = pltpu.make_async_copy(wo_ref.at[:, pl.ds(0, wide)], wbuf, loc_sem.at[7])
    ld_wo1 = pltpu.make_async_copy(wo_ref.at[:, pl.ds(wide, rest)], wo1, loc_sem.at[8])
    ld_x.start()
    ld_k.start()
    ld_v.start()
    lens[0] = jnp.full(lens.shape[1:], len_ref[0], jnp.int32)

    barrier = pltpu.get_barrier_semaphore()
    for other in (mate, peer):
        pl.semaphore_signal(barrier, inc=1, device_id={'cp': other}, device_id_type=MESH)
    pl.semaphore_wait(barrier, 2)

    my_rows = pl.ds(pl.multiple_of(core * tok, tok), tok)
    mate_rows = pl.ds(pl.multiple_of((1 - core) * tok, tok), tok)
    cp_x = remote(x_ref, xbuf.at[my_rows], pair_s.at[0], pair_r.at[0], mate)
    cp_len = remote(lens.at[0], lens.at[1], pair_s.at[1], pair_r.at[1], mate)
    cp_k = remote(k_ref.at[:, 1 - core], raw_k.at[1], pair_s.at[2], pair_r.at[2], mate)
    cp_v = remote(v_ref.at[:, 1 - core], raw_v.at[1], pair_s.at[3], pair_r.at[3], mate)
    cp_x.start()
    cp_len.start()
    for j in range(2):
        ld_wq(j).start()
    cp_k.start()
    cp_v.start()
    for j in range(2, n_chunk):
        ld_wq(j).start()
    ld_wk.start()
    ld_wv.start()
    ld_cos.start()
    ld_sin.start()

    row = lax.broadcasted_iota(jnp.int32, (2 * PREP, 2 * PREP), 0)
    col = lax.broadcasted_iota(jnp.int32, (2 * PREP, 2 * PREP), 1)
    want = jnp.where(row < PREP, 2 * row, 2 * (row - PREP) + 1)
    pick = jnp.where(col == want, 1.0, 0.0).astype(jnp.bfloat16)
    want_back = jnp.where(col < PREP, 2 * col, 2 * (col - PREP) + 1)
    weave = jnp.where(row == want_back, 1.0, 0.0).astype(jnp.bfloat16)
    lane = lax.broadcasted_iota(jnp.int32, (PREP, head_dim), 1)
    slot = lax.broadcasted_iota(jnp.int32, (PREP, head_dim), 0)

    def prep(block):
        flat_k = raw_k.at[block].reshape(2 * cache, head_dim)
        flat_v = raw_v.at[block].reshape(2 * cache, head_dim)

        def step(i, carry):
            for g in range(PREP_GROUPS):
                at = pl.multiple_of((i * PREP_GROUPS + g) * PREP, PREP)
                to = pl.multiple_of(block * cache + at, PREP)
                both = jnp.concatenate([flat_k[pl.ds(2 * at, 2 * PREP)], flat_v[pl.ds(2 * at, 2 * PREP)]], axis=1)
                split = jnp.dot(pick, both, preferred_element_type=jnp.float32).astype(jnp.bfloat16)
                hidden = jnp.where((slot + at >= lens[block, 0:1, :]) & (lane == 0), HIDE, 0.0).astype(jnp.bfloat16)
                for h in range(2):
                    part = split[h * PREP:(h + 1) * PREP]
                    kb[h, pl.ds(to, PREP), :head_dim] = part[:, :head_dim]
                    kb[h, pl.ds(to, PREP), head_dim:] = hidden
                    vt[h, :, pl.ds(to, PREP)] = part[:, head_dim:].T
            return carry

        lax.fori_loop(0, cache // PREP // PREP_GROUPS, step, 0)

    ld_k.wait()
    ld_v.wait()
    prep(0)

    def rope(vals):
        return vals * cosb[...] + pltpu.roll(vals, head_dim // 2, 1) * sinb[...]

    def cp_q(j):
        src = qbuf.at[pl.ds(2 * j, 2)]
        return remote(src, qbuf.at[pl.ds(my_heads + 2 * j, 2)], q_s.at[j], q_r.at[j], peer)

    ld_x.wait()
    ld_cos.wait()
    ld_sin.wait()
    cp_x.wait_recv()

    def project(first, count):
        return jnp.dot(xbuf[...], wbuf[:, pl.ds(pl.multiple_of(first * pair, pair), count * pair)], preferred_element_type=jnp.float32)

    def rotate(chunk, count):
        for j in range(count):
            for h in range(2):
                part = s_scr[chunk % 2, j * toks:(j + 1) * toks, h * head_dim:(h + 1) * head_dim]
                qbuf[4 * chunk + 2 * j + h] = rope(part).T.astype(jnp.bfloat16)

    def proj_step(c, carry):
        for j in (2 * c, 2 * c + 1):
            ld_wq(jnp.minimum(j, n_chunk - 1), j).wait()
        proj = project(2 * c, 2)
        rotate(jnp.maximum(c - 1, 0), 2)
        for n in range(2):
            s_scr[c % 2, n * toks:(n + 1) * toks] = proj[:, n * pair:(n + 1) * pair]

        @pl.when(c >= 1)
        def _():
            cp_q(2 * c - 2).start()
            cp_q(2 * c - 1).start()

        return carry

    n_proj = (n_chunk + 1) // 2
    lax.fori_loop(0, n_proj, proj_step, 0)
    last = n_proj - 1
    ld_wv.wait()
    v_proj = project(n_chunk + 1, 1)
    rotate(last, 1)
    cp_q(n_chunk - 1).start()
    ld_wo0.start()
    ld_wo1.start()
    k_heads = [rope(s_scr[last % 2, toks:2 * toks, h * head_dim:(h + 1) * head_dim]).astype(jnp.bfloat16) for h in range(2)]
    v_heads = [v_proj[:, h * head_dim:(h + 1) * head_dim].astype(jnp.bfloat16) for h in range(2)]
    for h in range(2):
        kn[h] = k_heads[h]
        vtn[h] = v_heads[h].T
    for part in range(2):
        rows = slice(part * tok, (part + 1) * tok)
        both = jnp.concatenate([jnp.concatenate([k_heads[h][rows], v_heads[h][rows]], axis=1) for h in range(2)], axis=0)
        mixed = jnp.dot(weave, both, preferred_element_type=jnp.float32).astype(jnp.bfloat16)
        for n in range(2):
            kvx[n, rows] = mixed[:, n * head_dim:(n + 1) * head_dim].reshape(tok, 2, head_dim)
    cp_ko = remote(kvx.at[0, mate_rows], kvr.at[0], pair_s.at[4], pair_r.at[4], mate)
    cp_vo = remote(kvx.at[1, mate_rows], kvr.at[1], pair_s.at[5], pair_r.at[5], mate)
    cp_ko.start()
    cp_vo.start()
    outs = [pltpu.make_async_copy(kvx.at[n, my_rows], out_ref.at[:, core], loc_sem.at[9 + n]) for n, out_ref in ((0, ko_ref), (1, vo_ref))]
    for out in outs:
        out.start()

    cp_len.wait_recv()
    cp_k.wait_recv()
    cp_v.wait_recv()
    prep(1)

    n_tiles = 2 * cache // KEY_TILE
    n_sub = KEY_TILE // SUB
    first_a = 2
    new_at = 3
    ones_row = jnp.where(lax.broadcasted_iota(jnp.int32, (head_dim, toks), 0) == 0, 1.0, 0.0).astype(jnp.bfloat16)

    def positions(chip_id, axis):
        within = lax.broadcasted_iota(jnp.int32, (toks, toks), axis)
        dev = 2 * chip_id + jnp.where(within >= tok, 1, 0)
        inner = jnp.where(within >= tok, within - tok, within)
        late = inner >= tok // 2
        piece_id = jnp.where(late, 2 * cp_size - 1 - dev, dev)
        return piece_id * (tok // 2) + jnp.where(late, inner - tok // 2, inner)

    def cp_p(h):
        return remote(ob.at[my_heads + h], pb.at[h], p_s.at[h], p_r.at[h], peer)

    def place(i):
        is_b = jnp.logical_and(i >= first_a, i < first_a + group)
        j = jnp.where(i < first_a, i, jnp.where(is_b, i - first_a, i - group))
        return is_b, jnp.where(is_b, my_heads + j, j), j

    def peak(s):
        return jnp.max(s.reshape(s.shape[0] // 8, 8, toks), axis=0)

    def scores(kvh, q_aug, t, r):
        s = jnp.dot(kb[kvh, t * KEY_TILE + r * SUB:t * KEY_TILE + (r + 1) * SUB], q_aug, preferred_element_type=jnp.float32)
        s_scr[t % 2, r * SUB:(r + 1) * SUB] = s
        return peak(s)

    def with_ones(q):
        return jnp.concatenate([q, ones_row], axis=0)

    def one_head(kvh, idx, next_kvh, next_idx, tops, q_chip):
        q_aug = with_ones(qbuf[idx])
        next_q = with_ones(qbuf[next_idx])
        tops = list(tops)
        top = None
        total = None
        for t in range(n_tiles):
            here = tops[t]
            if t == new_at:
                here = jnp.maximum(here, seg_tops)
            tile_top = jnp.max(here, axis=0, keepdims=True)
            new_top = tile_top if top is None else jnp.maximum(top, tile_top)
            keep = None if top is None else jnp.exp2((top - new_top) * score_c)
            top = new_top
            new_tops = None
            w_sum = None
            halves = []
            for r in range(n_sub):
                w = jnp.exp2((s_scr[t % 2, r * SUB:(r + 1) * SUB] - top) * score_c)
                if t + 2 < n_tiles:
                    sub_tops = scores(kvh, q_aug, t + 2, r)
                else:
                    sub_tops = scores(next_kvh, next_q, t + 2 - n_tiles, r)
                new_tops = sub_tops if new_tops is None else jnp.maximum(new_tops, sub_tops)
                part = jnp.sum(w.reshape(SUB // 8, 8, toks), axis=0)
                w_sum = part if w_sum is None else w_sum + part
                halves.append(w.astype(jnp.bfloat16))
                if len(halves) == PV_SUBS:
                    at = t * KEY_TILE + (r + 1 - PV_SUBS) * SUB
                    wide = halves[0] if PV_SUBS == 1 else jnp.concatenate(halves, axis=0)
                    halves = []
                    out = jnp.dot(vt[kvh, :, at:at + PV_SUBS * SUB], wide, preferred_element_type=jnp.float32)
                    if r + 1 > PV_SUBS:
                        acc[...] += out
                    elif keep is None:
                        acc[...] = out
                    else:
                        acc[...] = acc[...] * keep + out
            if t == new_at - 2:
                s = jnp.dot(kn[kvh], qbuf[idx], preferred_element_type=jnp.float32)
                s = jnp.where(positions(chip, 0) <= positions(q_chip, 1), s, -jnp.inf)
                sn_scr[...] = s
                seg_tops = peak(s)
            if t == new_at:
                w = jnp.exp2((sn_scr[...] - top) * score_c)
                w_sum = w_sum + jnp.sum(w.reshape(toks // 8, 8, toks), axis=0)
                acc[...] += jnp.dot(vtn[kvh], w.astype(jnp.bfloat16), preferred_element_type=jnp.float32)
            total = w_sum if keep is None else total * keep + w_sum
            tops.append(new_tops)
        ob[idx, :head_dim] = acc[...]
        ob[idx, head_dim:head_dim + 8] = jnp.broadcast_to(top, (8, toks))
        ob[idx, head_dim + 8:head_dim + 16] = jnp.broadcast_to(jnp.sum(total, axis=0, keepdims=True), (8, toks))

        return tops[n_tiles], tops[n_tiles + 1]

    def attend(i, tops):
        is_b, idx, j = place(i)
        q_chip = jnp.where(is_b, 1 - chip, chip)
        after = jnp.minimum(i + 1, 2 * group - 1)
        next_b, next_idx, next_j = place(after)
        fresh = jnp.logical_and(next_b, after > i)
        odd = lax.rem(next_j, 2) == 1

        @pl.when(jnp.logical_and(fresh, jnp.logical_and(jnp.logical_not(odd), next_j < group - 1)))
        def _():
            cp_q(lax.div(next_j, 2)).wait_recv()

        @pl.when(jnp.logical_and(fresh, odd))
        def _():
            cp_q(lax.div(next_j + group, 2)).wait_recv()

        @pl.when(jnp.logical_and(fresh, next_j == 0))
        def _():
            cp_q(group // 2).wait_recv()

        tops = one_head(0, idx, 1, idx + group, tops, q_chip)
        tops = one_head(1, idx + group, 0, next_idx, tops, q_chip)

        @pl.when(is_b)
        def _():
            cp_p(j).start()
            cp_p(j + group).start()

        return tops

    first_q = with_ones(qbuf[0])
    start_tops = []
    for t in range(2):
        tops = scores(0, first_q, t, 0)
        for r in range(1, n_sub):
            tops = jnp.maximum(tops, scores(0, first_q, t, r))
        start_tops.append(tops)
    lax.fori_loop(0, 2 * group, attend, tuple(start_tops))

    cp_ko.wait()
    cp_vo.wait()
    more = [pltpu.make_async_copy(kvr.at[n], out_ref.at[:, 1 - core], loc_sem.at[11 + n]) for n, out_ref in ((0, ko_ref), (1, vo_ref))]
    for out in more:
        out.start()

    def cp_o(h):
        col = pl.multiple_of((core * my_heads + h) * head_dim, head_dim)
        return remote(ost.at[h, mate_rows], oall.at[:, pl.ds(col, head_dim)], o_s.at[h], o_r.at[h], mate)

    def combine(h, carry):
        cp_p(h).wait_recv()
        top_a, top_b = ob[h, head_dim:head_dim + 1], pb[h, head_dim:head_dim + 1]
        top = jnp.maximum(top_a, top_b)
        keep_a = jnp.exp2((top_a - top) * score_c)
        keep_b = jnp.exp2((top_b - top) * score_c)
        total = ob[h, head_dim + 8:head_dim + 9] * keep_a + pb[h, head_dim + 8:head_dim + 9] * keep_b
        out = (ob[h, :head_dim] * keep_a + pb[h, :head_dim] * keep_b) / total
        ost[h] = out.T.astype(jnp.bfloat16)
        cp_o(h).start()
        col = pl.multiple_of((core * my_heads + h) * head_dim, head_dim)
        oall[:, pl.ds(col, head_dim)] = ost[h, my_rows]
        return carry

    lax.fori_loop(0, my_heads, combine, 0)
    ld_wo0.wait()
    ld_wo1.wait()

    own = pl.ds(pl.multiple_of(core * half_cols, half_cols), half_cols)
    other = pl.ds(pl.multiple_of((1 - core) * half_cols, half_cols), half_cols)
    spans = [(wbuf, n * pair, n * pair) for n in range(wide // pair)] + [(wo1, n * pair, wide + n * pair) for n in range(rest // pair)]

    def y_part(weights, at, rows):
        return jnp.dot(oall[:, rows], weights[rows, at:at + pair], preferred_element_type=jnp.float32)

    for n, (weights, at, _) in enumerate(spans):
        s_scr[n // 8, (n % 8) * tok:(n % 8 + 1) * tok] = y_part(weights, at, own)

    def drain(h, carry):
        cp_o(h).wait()
        cp_p(h).wait_send()
        return carry

    lax.fori_loop(0, my_heads, drain, 0)
    y_copies = []
    cuts = [len(spans) // 2, len(spans)]
    for n, (weights, at, col) in enumerate(spans):
        part = s_scr[n // 8, (n % 8) * tok:(n % 8 + 1) * tok] + y_part(weights, at, other)
        ybuf[:, col:col + pair] = part.astype(jnp.bfloat16)
        if n + 1 in cuts:
            which = cuts.index(n + 1)
            first = 0 if which == 0 else spans[cuts[which - 1]][2]
            cols = pl.ds(first, col + pair - first)
            y_copies.append(pltpu.make_async_copy(ybuf.at[:, cols], y_ref.at[:, cols], loc_sem.at[13 + which]))
            y_copies[-1].start()
    for out in y_copies + outs + more:
        out.wait()
    for j in range(n_chunk):
        cp_q(j).wait_send()
    for copy in (cp_x, cp_len, cp_k, cp_v):
        copy.wait_send()


def hand_on(y_in, k_in, v_in, y_ref, k_ref, v_ref, y_buf, k_buf, v_buf, in_sem, out_sem):
    rows = y_in.shape[0] // 4
    parts = [(src.at[...], buf.at[...], dst.at[...]) for src, buf, dst in ((k_in, k_buf, k_ref), (v_in, v_buf, v_ref))]
    for n in range(4):
        cut = pl.ds(n * rows, rows)
        parts.append((y_in.at[cut], y_buf.at[cut], y_ref.at[cut]))
    loads = [pltpu.make_async_copy(src, buf, in_sem.at[n]) for n, (src, buf, _) in enumerate(parts)]
    stores = [pltpu.make_async_copy(buf, dst, out_sem.at[n]) for n, (_, buf, dst) in enumerate(parts)]
    for load in loads:
        load.start()
    for load, store in zip(loads, stores):
        load.wait()
        store.start()
    for store in stores:
        store.wait()


def solution(mesh):
    cp_size = mesh.shape['cp']
    row_spec = P(('dp', 'cp'), None)
    cache_spec = P(('dp', 'cp'), None, None)
    len_spec = P(('dp', 'cp'))
    full_spec = P()

    def device_fn(x_new, k_cache, v_cache, valid_len, w_q, w_k, w_v, w_o):
        tok, width = x_new.shape
        cache, kv_heads, head_dim = k_cache.shape
        heads = w_q.shape[1] // head_dim
        my_heads = heads // 2
        toks = 2 * tok
        half_cols = my_heads * head_dim
        cos, sin = rope_constants(tok, cp_size, cache * cp_size, head_dim)
        dims = (heads, head_dim, heads // kv_heads, tok, cache, cp_size)
        bf16, f32 = jnp.bfloat16, jnp.float32
        k4 = k_cache.reshape(cache, 2, 2, head_dim)
        v4 = v_cache.reshape(cache, 2, 2, head_dim)
        any_spec = pl.BlockSpec(memory_space=pl.ANY)
        dma = pltpu.SemaphoreType.DMA
        y_out, k_new, v_new = pl.pallas_call(
            functools.partial(kernel, dims),
            out_shape=(
                jax.ShapeDtypeStruct((tok, width), bf16),
                jax.ShapeDtypeStruct((tok, kv_heads // 2, 2, head_dim), bf16),
                jax.ShapeDtypeStruct((tok, kv_heads // 2, 2, head_dim), bf16),
            ),
            in_specs=[pl.BlockSpec(memory_space=pltpu.SMEM)] + [any_spec] * 9,
            out_specs=(any_spec,) * 3,
            scratch_shapes=[
                pltpu.VMEM((toks, width), bf16),
                pltpu.VMEM((2, cache, 2, head_dim), bf16),
                pltpu.VMEM((2, cache, 2, head_dim), bf16),
                pltpu.VMEM((2, 8, head_dim), jnp.int32),
                pltpu.VMEM((2, 2 * cache, 2 * head_dim), bf16),
                pltpu.VMEM((2, head_dim, 2 * cache), bf16),
                pltpu.VMEM((2, toks, head_dim), bf16),
                pltpu.VMEM((2, head_dim, toks), bf16),
                pltpu.VMEM((width, half_cols + 4 * head_dim), bf16),
                pltpu.VMEM((width, heads * head_dim - half_cols - 4 * head_dim), bf16),
                pltpu.VMEM((toks, head_dim), f32),
                pltpu.VMEM((toks, head_dim), f32),
                pltpu.VMEM((heads, head_dim, toks), bf16),
                pltpu.VMEM((heads, head_dim + 16, toks), f32),
                pltpu.VMEM((my_heads, head_dim + 16, toks), f32),
                pltpu.VMEM((tok, heads * head_dim), bf16),
                pltpu.VMEM((my_heads, toks, head_dim), bf16),
                pltpu.VMEM((2, toks, 2, head_dim), bf16),
                pltpu.VMEM((2, tok, 2, head_dim), bf16),
                pltpu.VMEM((tok, width), bf16),
                pltpu.VMEM((2, KEY_TILE, toks), f32),
                pltpu.VMEM((toks, toks), f32),
                pltpu.VMEM((head_dim, toks), f32),
                dma((15,)), dma((my_heads // 2 + 2,)), dma((6,)), dma((6,)),
                dma((my_heads // 2,)), dma((my_heads // 2,)),
                dma((my_heads,)), dma((my_heads,)), dma((my_heads,)), dma((my_heads,)),
            ],
            compiler_params=pltpu.CompilerParams(collective_id=0, has_side_effects=True, vmem_limit_bytes=67043328),
        )(valid_len, x_new, k4, v4, w_q, w_k, w_v, w_o, jnp.asarray(cos), jnp.asarray(sin))
        y_out, k_new, v_new = pl.pallas_call(
            hand_on,
            out_shape=tuple(jax.ShapeDtypeStruct(part.shape, bf16) for part in (y_out, k_new, v_new)),
            in_specs=[any_spec] * 3,
            out_specs=(any_spec,) * 3,
            scratch_shapes=[pltpu.VMEM(part.shape, bf16) for part in (y_out, k_new, v_new)] + [dma((6,)), dma((6,))],
        )(y_out, k_new, v_new)
        shape = (tok, kv_heads, head_dim)
        return y_out, k_new.reshape(shape), v_new.reshape(shape)

    return jax.shard_map(device_fn, mesh=mesh, in_specs=(row_spec, cache_spec, cache_spec, len_spec, full_spec, full_spec, full_spec, full_spec), out_specs=(row_spec, cache_spec, cache_spec), check_vma=False)
```

```python
import functools
import math

import jax
import jax.numpy as jnp
import numpy as np
from jax import lax
from jax.experimental import pallas as pl
from jax.experimental.pallas import tpu as pltpu
from jax.sharding import PartitionSpec as P

ROPE_BASE = 500000.0
MESH = pl.DeviceIdType.MESH
KEY_TILE = 1024
SUB = 1024
PV_SUBS = 1
PREP = 128
PREP_GROUPS = 4
HIDE = -3e38


def rope_constants(tok_dev, cp_size, cache_len, head_dim):
    piece = tok_dev // 2
    half = head_dim // 2
    inv_freq = ROPE_BASE ** (-np.arange(half, dtype=np.float64) * 2.0 / head_dim)
    within = np.arange(tok_dev)
    rows = []
    for dev in range(cp_size):
        piece_ids = np.where(within < piece, dev, 2 * cp_size - 1 - dev)
        rows.append(cache_len + piece_ids * piece + within % piece)
    angles = np.concatenate(rows).astype(np.float64)[:, None] * inv_freq[None, :]
    cos, sin = np.cos(angles), np.sin(angles)
    cos_full = np.concatenate([cos, cos], axis=1).astype(np.float32)
    sin_full = np.concatenate([-sin, sin], axis=1).astype(np.float32)
    shape = (cp_size // 2, 2 * tok_dev, head_dim)
    return cos_full.reshape(shape), sin_full.reshape(shape)


def dot_t(lhs, rhs):
    return lax.dot_general(lhs, rhs, (((1,), (1,)), ((), ())), preferred_element_type=jnp.float32)


def kernel(dims, len_ref, x_ref, k_ref, v_ref, wq_ref, wk_ref, wv_ref, wo_ref, cos_ref, sin_ref, y_ref, ko_ref, vo_ref,
           xbuf, raw_k, raw_v, lens, kb, vt, kn, vtn, wbuf, wo1, cosb, sinb, qbuf, ob, pb, oall, ost, kvx, kvr, ybuf, s_scr, sn_scr, acc,
           loc_sem, wq_sem, pair_s, pair_r, q_s, q_r, p_s, p_r, o_s, o_r):
    heads, head_dim, group, tok, cache, cp_size = dims
    my_heads = heads // 2
    half_cols = my_heads * head_dim
    toks = 2 * tok
    pair = 2 * head_dim
    score_c = math.log2(math.e) / math.sqrt(head_dim)

    me = lax.axis_index('cp')
    core = lax.rem(me, 2)
    chip = lax.div(me, 2)
    mate = me + 1 - 2 * core
    peer = lax.rem(me + 2, cp_size)

    def remote(src, dst, send, recv, dev):
        return pltpu.make_async_remote_copy(src_ref=src, dst_ref=dst, send_sem=send, recv_sem=recv, device_id={'cp': dev}, device_id_type=MESH)

    ld_x = pltpu.make_async_copy(x_ref, xbuf.at[pl.ds(pl.multiple_of(core * tok, tok), tok)], loc_sem.at[0])
    ld_cos = pltpu.make_async_copy(cos_ref.at[chip], cosb, loc_sem.at[1])
    ld_sin = pltpu.make_async_copy(sin_ref.at[chip], sinb, loc_sem.at[2])
    ld_k = pltpu.make_async_copy(k_ref.at[:, core], raw_k.at[0], loc_sem.at[3])
    ld_v = pltpu.make_async_copy(v_ref.at[:, core], raw_v.at[0], loc_sem.at[4])
    n_chunk = my_heads // 2

    def ld_wq(j, sem=None):
        sem = j if sem is None else sem
        col = pl.multiple_of(core * half_cols + j * pair, pair)
        return pltpu.make_async_copy(wq_ref.at[:, pl.ds(col, pair)], wbuf.at[:, pl.ds(pl.multiple_of(j * pair, pair), pair)], wq_sem.at[sem])

    kv_col = pl.multiple_of(core * pair, pair)
    ld_wk = pltpu.make_async_copy(wk_ref.at[:, pl.ds(kv_col, pair)], wbuf.at[:, pl.ds(half_cols, pair)], wq_sem.at[n_chunk])
    ld_wv = pltpu.make_async_copy(wv_ref.at[:, pl.ds(kv_col, pair)], wbuf.at[:, pl.ds(half_cols + pair, pair)], wq_sem.at[n_chunk + 1])
    wide = wbuf.shape[1]
    rest = wo1.shape[1]
    ld_wo0 = pltpu.make_async_copy(wo_ref.at[:, pl.ds(0, wide)], wbuf, loc_sem.at[7])
    ld_wo1 = pltpu.make_async_copy(wo_ref.at[:, pl.ds(wide, rest)], wo1, loc_sem.at[8])
    ld_x.start()
    ld_k.start()
    ld_v.start()
    lens[0] = jnp.full(lens.shape[1:], len_ref[0], jnp.int32)

    barrier = pltpu.get_barrier_semaphore()
    for other in (mate, peer):
        pl.semaphore_signal(barrier, inc=1, device_id={'cp': other}, device_id_type=MESH)
    pl.semaphore_wait(barrier, 2)

    my_rows = pl.ds(pl.multiple_of(core * tok, tok), tok)
    mate_rows = pl.ds(pl.multiple_of((1 - core) * tok, tok), tok)
    cp_x = remote(x_ref, xbuf.at[my_rows], pair_s.at[0], pair_r.at[0], mate)
    cp_len = remote(lens.at[0], lens.at[1], pair_s.at[1], pair_r.at[1], mate)
    cp_k = remote(k_ref.at[:, 1 - core], raw_k.at[1], pair_s.at[2], pair_r.at[2], mate)
    cp_v = remote(v_ref.at[:, 1 - core], raw_v.at[1], pair_s.at[3], pair_r.at[3], mate)
    cp_x.start()
    cp_len.start()
    for j in range(2):
        ld_wq(j).start()
    cp_k.start()
    cp_v.start()
    for j in range(2, n_chunk):
        ld_wq(j).start()
    ld_wk.start()
    ld_wv.start()
    ld_cos.start()
    ld_sin.start()

    row = lax.broadcasted_iota(jnp.int32, (2 * PREP, 2 * PREP), 0)
    col = lax.broadcasted_iota(jnp.int32, (2 * PREP, 2 * PREP), 1)
    want = jnp.where(row < PREP, 2 * row, 2 * (row - PREP) + 1)
    pick = jnp.where(col == want, 1.0, 0.0).astype(jnp.bfloat16)
    want_back = jnp.where(col < PREP, 2 * col, 2 * (col - PREP) + 1)
    weave = jnp.where(row == want_back, 1.0, 0.0).astype(jnp.bfloat16)
    lane = lax.broadcasted_iota(jnp.int32, (PREP, head_dim), 1)
    slot = lax.broadcasted_iota(jnp.int32, (PREP, head_dim), 0)

    def prep(block):
        flat_k = raw_k.at[block].reshape(2 * cache, head_dim)
        flat_v = raw_v.at[block].reshape(2 * cache, head_dim)

        def step(i, carry):
            for g in range(PREP_GROUPS):
                at = pl.multiple_of((i * PREP_GROUPS + g) * PREP, PREP)
                to = pl.multiple_of(block * cache + at, PREP)
                both = jnp.concatenate([flat_k[pl.ds(2 * at, 2 * PREP)], flat_v[pl.ds(2 * at, 2 * PREP)]], axis=1)
                split = jnp.dot(pick, both, preferred_element_type=jnp.float32).astype(jnp.bfloat16)
                hidden = jnp.where((slot + at >= lens[block, 0:1, :]) & (lane == 0), HIDE, 0.0).astype(jnp.bfloat16)
                for h in range(2):
                    part = split[h * PREP:(h + 1) * PREP]
                    kb[h, pl.ds(to, PREP), :head_dim] = part[:, :head_dim]
                    kb[h, pl.ds(to, PREP), head_dim:] = hidden
                    vt[h, :, pl.ds(to, PREP)] = part[:, head_dim:].T
            return carry

        lax.fori_loop(0, cache // PREP // PREP_GROUPS, step, 0)

    ld_k.wait()
    ld_v.wait()
    prep(0)

    def rope(vals):
        return vals * cosb[...] + pltpu.roll(vals, head_dim // 2, 1) * sinb[...]

    def cp_q(j):
        src = qbuf.at[pl.ds(2 * j, 2)]
        return remote(src, qbuf.at[pl.ds(my_heads + 2 * j, 2)], q_s.at[j], q_r.at[j], peer)

    ld_x.wait()
    ld_cos.wait()
    ld_sin.wait()
    cp_x.wait_recv()

    def project(first, count):
        return jnp.dot(xbuf[...], wbuf[:, pl.ds(pl.multiple_of(first * pair, pair), count * pair)], preferred_element_type=jnp.float32)

    def rotate(chunk, count):
        for j in range(count):
            for h in range(2):
                part = s_scr[chunk % 2, j * toks:(j + 1) * toks, h * head_dim:(h + 1) * head_dim]
                qbuf[4 * chunk + 2 * j + h] = rope(part).T.astype(jnp.bfloat16)

    def proj_step(c, carry):
        for j in (2 * c, 2 * c + 1):
            ld_wq(jnp.minimum(j, n_chunk - 1), j).wait()
        proj = project(2 * c, 2)
        rotate(jnp.maximum(c - 1, 0), 2)
        for n in range(2):
            s_scr[c % 2, n * toks:(n + 1) * toks] = proj[:, n * pair:(n + 1) * pair]

        @pl.when(c >= 1)
        def _():
            cp_q(2 * c - 2).start()
            cp_q(2 * c - 1).start()

        return carry

    n_proj = (n_chunk + 1) // 2
    lax.fori_loop(0, n_proj, proj_step, 0)
    last = n_proj - 1
    ld_wv.wait()
    v_proj = project(n_chunk + 1, 1)
    rotate(last, 1)
    cp_q(n_chunk - 1).start()
    ld_wo0.start()
    ld_wo1.start()
    k_heads = [rope(s_scr[last % 2, toks:2 * toks, h * head_dim:(h + 1) * head_dim]).astype(jnp.bfloat16) for h in range(2)]
    v_heads = [v_proj[:, h * head_dim:(h + 1) * head_dim].astype(jnp.bfloat16) for h in range(2)]
    for h in range(2):
        kn[h] = k_heads[h]
        vtn[h] = v_heads[h].T
    for part in range(2):
        rows = slice(part * tok, (part + 1) * tok)
        both = jnp.concatenate([jnp.concatenate([k_heads[h][rows], v_heads[h][rows]], axis=1) for h in range(2)], axis=0)
        mixed = jnp.dot(weave, both, preferred_element_type=jnp.float32).astype(jnp.bfloat16)
        for n in range(2):
            kvx[n, rows] = mixed[:, n * head_dim:(n + 1) * head_dim].reshape(tok, 2, head_dim)
    cp_ko = remote(kvx.at[0, mate_rows], kvr.at[0], pair_s.at[4], pair_r.at[4], mate)
    cp_vo = remote(kvx.at[1, mate_rows], kvr.at[1], pair_s.at[5], pair_r.at[5], mate)
    cp_ko.start()
    cp_vo.start()
    outs = [pltpu.make_async_copy(kvx.at[n, my_rows], out_ref.at[:, core], loc_sem.at[9 + n]) for n, out_ref in ((0, ko_ref), (1, vo_ref))]
    for out in outs:
        out.start()

    cp_len.wait_recv()
    cp_k.wait_recv()
    cp_v.wait_recv()
    prep(1)

    n_tiles = 2 * cache // KEY_TILE
    n_sub = KEY_TILE // SUB
    first_a = 2
    new_at = 3
    ones_row = jnp.where(lax.broadcasted_iota(jnp.int32, (head_dim, toks), 0) == 0, 1.0, 0.0).astype(jnp.bfloat16)

    def positions(chip_id, axis):
        within = lax.broadcasted_iota(jnp.int32, (toks, toks), axis)
        dev = 2 * chip_id + jnp.where(within >= tok, 1, 0)
        inner = jnp.where(within >= tok, within - tok, within)
        late = inner >= tok // 2
        piece_id = jnp.where(late, 2 * cp_size - 1 - dev, dev)
        return piece_id * (tok // 2) + jnp.where(late, inner - tok // 2, inner)

    def cp_p(h):
        return remote(ob.at[my_heads + h], pb.at[h], p_s.at[h], p_r.at[h], peer)

    def place(i):
        is_b = jnp.logical_and(i >= first_a, i < first_a + group)
        j = jnp.where(i < first_a, i, jnp.where(is_b, i - first_a, i - group))
        return is_b, jnp.where(is_b, my_heads + j, j), j

    def peak(s):
        return jnp.max(s.reshape(s.shape[0] // 8, 8, toks), axis=0)

    def scores(kvh, q_aug, t, r):
        s = jnp.dot(kb[kvh, t * KEY_TILE + r * SUB:t * KEY_TILE + (r + 1) * SUB], q_aug, preferred_element_type=jnp.float32)
        s_scr[t % 2, r * SUB:(r + 1) * SUB] = s
        return peak(s)

    def with_ones(q):
        return jnp.concatenate([q, ones_row], axis=0)

    def one_head(kvh, idx, next_kvh, next_idx, tops, q_chip):
        q_aug = with_ones(qbuf[idx])
        next_q = with_ones(qbuf[next_idx])
        tops = list(tops)
        top = None
        total = None
        for t in range(n_tiles):
            here = tops[t]
            if t == new_at:
                here = jnp.maximum(here, seg_tops)
            tile_top = jnp.max(here, axis=0, keepdims=True)
            new_top = tile_top if top is None else jnp.maximum(top, tile_top)
            keep = None if top is None else jnp.exp2((top - new_top) * score_c)
            top = new_top
            new_tops = None
            w_sum = None
            halves = []
            for r in range(n_sub):
                w = jnp.exp2((s_scr[t % 2, r * SUB:(r + 1) * SUB] - top) * score_c)
                if t + 2 < n_tiles:
                    sub_tops = scores(kvh, q_aug, t + 2, r)
                else:
                    sub_tops = scores(next_kvh, next_q, t + 2 - n_tiles, r)
                new_tops = sub_tops if new_tops is None else jnp.maximum(new_tops, sub_tops)
                part = jnp.sum(w.reshape(SUB // 8, 8, toks), axis=0)
                w_sum = part if w_sum is None else w_sum + part
                halves.append(w.astype(jnp.bfloat16))
                if len(halves) == PV_SUBS:
                    at = t * KEY_TILE + (r + 1 - PV_SUBS) * SUB
                    wide = halves[0] if PV_SUBS == 1 else jnp.concatenate(halves, axis=0)
                    halves = []
                    out = jnp.dot(vt[kvh, :, at:at + PV_SUBS * SUB], wide, preferred_element_type=jnp.float32)
                    if r + 1 > PV_SUBS:
                        acc[...] += out
                    elif keep is None:
                        acc[...] = out
                    else:
                        acc[...] = acc[...] * keep + out
            if t == new_at - 2:
                s = jnp.dot(kn[kvh], qbuf[idx], preferred_element_type=jnp.float32)
                s = jnp.where(positions(chip, 0) <= positions(q_chip, 1), s, -jnp.inf)
                sn_scr[...] = s
                seg_tops = peak(s)
            if t == new_at:
                w = jnp.exp2((sn_scr[...] - top) * score_c)
                w_sum = w_sum + jnp.sum(w.reshape(toks // 8, 8, toks), axis=0)
                acc[...] += jnp.dot(vtn[kvh], w.astype(jnp.bfloat16), preferred_element_type=jnp.float32)
            total = w_sum if keep is None else total * keep + w_sum
            tops.append(new_tops)
        ob[idx, :head_dim] = acc[...]
        ob[idx, head_dim:head_dim + 8] = jnp.broadcast_to(top, (8, toks))
        ob[idx, head_dim + 8:head_dim + 16] = jnp.broadcast_to(jnp.sum(total, axis=0, keepdims=True), (8, toks))

        return tops[n_tiles], tops[n_tiles + 1]

    def attend(i, tops):
        is_b, idx, j = place(i)
        q_chip = jnp.where(is_b, 1 - chip, chip)
        after = jnp.minimum(i + 1, 2 * group - 1)
        next_b, next_idx, next_j = place(after)
        fresh = jnp.logical_and(next_b, after > i)
        odd = lax.rem(next_j, 2) == 1

        @pl.when(jnp.logical_and(fresh, jnp.logical_and(jnp.logical_not(odd), next_j < group - 1)))
        def _():
            cp_q(lax.div(next_j, 2)).wait_recv()

        @pl.when(jnp.logical_and(fresh, odd))
        def _():
            cp_q(lax.div(next_j + group, 2)).wait_recv()

        @pl.when(jnp.logical_and(fresh, next_j == 0))
        def _():
            cp_q(group // 2).wait_recv()

        tops = one_head(0, idx, 1, idx + group, tops, q_chip)
        tops = one_head(1, idx + group, 0, next_idx, tops, q_chip)

        @pl.when(is_b)
        def _():
            cp_p(j).start()
            cp_p(j + group).start()

        return tops

    first_q = with_ones(qbuf[0])
    start_tops = []
    for t in range(2):
        tops = scores(0, first_q, t, 0)
        for r in range(1, n_sub):
            tops = jnp.maximum(tops, scores(0, first_q, t, r))
        start_tops.append(tops)
    lax.fori_loop(0, 2 * group, attend, tuple(start_tops))

    cp_ko.wait()
    cp_vo.wait()
    more = [pltpu.make_async_copy(kvr.at[n], out_ref.at[:, 1 - core], loc_sem.at[11 + n]) for n, out_ref in ((0, ko_ref), (1, vo_ref))]
    for out in more:
        out.start()

    def cp_o(h):
        col = pl.multiple_of((core * my_heads + h) * head_dim, head_dim)
        return remote(ost.at[h, mate_rows], oall.at[:, pl.ds(col, head_dim)], o_s.at[h], o_r.at[h], mate)

    def combine_one(h):
        top_a, top_b = ob[h, head_dim:head_dim + 1], pb[h, head_dim:head_dim + 1]
        top = jnp.maximum(top_a, top_b)
        keep_a = jnp.exp2((top_a - top) * score_c)
        keep_b = jnp.exp2((top_b - top) * score_c)
        total = ob[h, head_dim + 8:head_dim + 9] * keep_a + pb[h, head_dim + 8:head_dim + 9] * keep_b
        out = (ob[h, :head_dim] * keep_a + pb[h, :head_dim] * keep_b) / total
        ost[h] = out.T.astype(jnp.bfloat16)
        col = pl.multiple_of((core * my_heads + h) * head_dim, head_dim)
        oall[:, pl.ds(col, head_dim)] = ost[h, my_rows]

    def combine(j, carry):
        for h in range(group):
            cp_p(j * group + h).wait_recv()
        for h in range(group):
            combine_one(j * group + h)
        for h in range(group):
            cp_o(j * group + h).start()
        return carry

    lax.fori_loop(0, 2, combine, 0)
    ld_wo0.wait()
    ld_wo1.wait()

    own = pl.ds(pl.multiple_of(core * half_cols, half_cols), half_cols)
    other = pl.ds(pl.multiple_of((1 - core) * half_cols, half_cols), half_cols)
    spans = [(wbuf, n * pair, n * pair) for n in range(wide // pair)] + [(wo1, n * pair, wide + n * pair) for n in range(rest // pair)]

    def y_part(weights, at, rows):
        return jnp.dot(oall[:, rows], weights[rows, at:at + pair], preferred_element_type=jnp.float32)

    for n, (weights, at, _) in enumerate(spans):
        s_scr[n // 8, (n % 8) * tok:(n % 8 + 1) * tok] = y_part(weights, at, own)

    def drain(h, carry):
        cp_o(h).wait()
        cp_p(h).wait_send()
        return carry

    lax.fori_loop(0, my_heads, drain, 0)
    y_copies = []
    cuts = [len(spans) // 2, len(spans)]
    for n, (weights, at, col) in enumerate(spans):
        part = s_scr[n // 8, (n % 8) * tok:(n % 8 + 1) * tok] + y_part(weights, at, other)
        ybuf[:, col:col + pair] = part.astype(jnp.bfloat16)
        if n + 1 in cuts:
            which = cuts.index(n + 1)
            first = 0 if which == 0 else spans[cuts[which - 1]][2]
            cols = pl.ds(first, col + pair - first)
            y_copies.append(pltpu.make_async_copy(ybuf.at[:, cols], y_ref.at[:, cols], loc_sem.at[13 + which]))
            y_copies[-1].start()
    for out in y_copies + outs + more:
        out.wait()
    for j in range(n_chunk):
        cp_q(j).wait_send()
    for copy in (cp_x, cp_len, cp_k, cp_v):
        copy.wait_send()


def hand_on(y_in, k_in, v_in, y_ref, k_ref, v_ref, y_buf, k_buf, v_buf, in_sem, out_sem):
    rows = y_in.shape[0] // 4
    parts = [(src.at[...], buf.at[...], dst.at[...]) for src, buf, dst in ((k_in, k_buf, k_ref), (v_in, v_buf, v_ref))]
    for n in range(4):
        cut = pl.ds(n * rows, rows)
        parts.append((y_in.at[cut], y_buf.at[cut], y_ref.at[cut]))
    loads = [pltpu.make_async_copy(src, buf, in_sem.at[n]) for n, (src, buf, _) in enumerate(parts)]
    stores = [pltpu.make_async_copy(buf, dst, out_sem.at[n]) for n, (_, buf, dst) in enumerate(parts)]
    for load in loads:
        load.start()
    for load, store in zip(loads, stores):
        load.wait()
        store.start()
    for store in stores:
        store.wait()


def solution(mesh):
    cp_size = mesh.shape['cp']
    row_spec = P(('dp', 'cp'), None)
    cache_spec = P(('dp', 'cp'), None, None)
    len_spec = P(('dp', 'cp'))
    full_spec = P()

    def device_fn(x_new, k_cache, v_cache, valid_len, w_q, w_k, w_v, w_o):
        tok, width = x_new.shape
        cache, kv_heads, head_dim = k_cache.shape
        heads = w_q.shape[1] // head_dim
        my_heads = heads // 2
        toks = 2 * tok
        half_cols = my_heads * head_dim
        cos, sin = rope_constants(tok, cp_size, cache * cp_size, head_dim)
        dims = (heads, head_dim, heads // kv_heads, tok, cache, cp_size)
        bf16, f32 = jnp.bfloat16, jnp.float32
        k4 = k_cache.reshape(cache, 2, 2, head_dim)
        v4 = v_cache.reshape(cache, 2, 2, head_dim)
        any_spec = pl.BlockSpec(memory_space=pl.ANY)
        dma = pltpu.SemaphoreType.DMA
        y_out, k_new, v_new = pl.pallas_call(
            functools.partial(kernel, dims),
            out_shape=(
                jax.ShapeDtypeStruct((tok, width), bf16),
                jax.ShapeDtypeStruct((tok, kv_heads // 2, 2, head_dim), bf16),
                jax.ShapeDtypeStruct((tok, kv_heads // 2, 2, head_dim), bf16),
            ),
            in_specs=[pl.BlockSpec(memory_space=pltpu.SMEM)] + [any_spec] * 9,
            out_specs=(any_spec,) * 3,
            scratch_shapes=[
                pltpu.VMEM((toks, width), bf16),
                pltpu.VMEM((2, cache, 2, head_dim), bf16),
                pltpu.VMEM((2, cache, 2, head_dim), bf16),
                pltpu.VMEM((2, 8, head_dim), jnp.int32),
                pltpu.VMEM((2, 2 * cache, 2 * head_dim), bf16),
                pltpu.VMEM((2, head_dim, 2 * cache), bf16),
                pltpu.VMEM((2, toks, head_dim), bf16),
                pltpu.VMEM((2, head_dim, toks), bf16),
                pltpu.VMEM((width, half_cols + 4 * head_dim), bf16),
                pltpu.VMEM((width, heads * head_dim - half_cols - 4 * head_dim), bf16),
                pltpu.VMEM((toks, head_dim), f32),
                pltpu.VMEM((toks, head_dim), f32),
                pltpu.VMEM((heads, head_dim, toks), bf16),
                pltpu.VMEM((heads, head_dim + 16, toks), f32),
                pltpu.VMEM((my_heads, head_dim + 16, toks), f32),
                pltpu.VMEM((tok, heads * head_dim), bf16),
                pltpu.VMEM((my_heads, toks, head_dim), bf16),
                pltpu.VMEM((2, toks, 2, head_dim), bf16),
                pltpu.VMEM((2, tok, 2, head_dim), bf16),
                pltpu.VMEM((tok, width), bf16),
                pltpu.VMEM((2, KEY_TILE, toks), f32),
                pltpu.VMEM((toks, toks), f32),
                pltpu.VMEM((head_dim, toks), f32),
                dma((15,)), dma((my_heads // 2 + 2,)), dma((6,)), dma((6,)),
                dma((my_heads // 2,)), dma((my_heads // 2,)),
                dma((my_heads,)), dma((my_heads,)), dma((my_heads,)), dma((my_heads,)),
            ],
            compiler_params=pltpu.CompilerParams(collective_id=0, has_side_effects=True, vmem_limit_bytes=67043328),
        )(valid_len, x_new, k4, v4, w_q, w_k, w_v, w_o, jnp.asarray(cos), jnp.asarray(sin))
        y_out, k_new, v_new = pl.pallas_call(
            hand_on,
            out_shape=tuple(jax.ShapeDtypeStruct(part.shape, bf16) for part in (y_out, k_new, v_new)),
            in_specs=[any_spec] * 3,
            out_specs=(any_spec,) * 3,
            scratch_shapes=[pltpu.VMEM(part.shape, bf16) for part in (y_out, k_new, v_new)] + [dma((6,)), dma((6,))],
        )(y_out, k_new, v_new)
        shape = (tok, kv_heads, head_dim)
        return y_out, k_new.reshape(shape), v_new.reshape(shape)

    return jax.shard_map(device_fn, mesh=mesh, in_specs=(row_spec, cache_spec, cache_spec, len_spec, full_spec, full_spec, full_spec, full_spec), out_specs=(row_spec, cache_spec, cache_spec), check_vma=False)
```

```python
import functools
import math

import jax
import jax.numpy as jnp
import numpy as np
from jax import lax
from jax.experimental import pallas as pl
from jax.experimental.pallas import tpu as pltpu
from jax.sharding import PartitionSpec as P

ROPE_BASE = 500000.0
MESH = pl.DeviceIdType.MESH
KEY_TILE = 1024
SUB = 1024
PV_SUBS = 1
PREP = 128
PREP_GROUPS = 4
HIDE = -3e38


def rope_constants(tok_dev, cp_size, cache_len, head_dim):
    piece = tok_dev // 2
    half = head_dim // 2
    inv_freq = ROPE_BASE ** (-np.arange(half, dtype=np.float64) * 2.0 / head_dim)
    within = np.arange(tok_dev)
    rows = []
    for dev in range(cp_size):
        piece_ids = np.where(within < piece, dev, 2 * cp_size - 1 - dev)
        rows.append(cache_len + piece_ids * piece + within % piece)
    angles = np.concatenate(rows).astype(np.float64)[:, None] * inv_freq[None, :]
    cos, sin = np.cos(angles), np.sin(angles)
    cos_full = np.concatenate([cos, cos], axis=1).astype(np.float32)
    sin_full = np.concatenate([-sin, sin], axis=1).astype(np.float32)
    shape = (cp_size // 2, 2 * tok_dev, head_dim)
    return cos_full.reshape(shape), sin_full.reshape(shape)


def dot_t(lhs, rhs):
    return lax.dot_general(lhs, rhs, (((1,), (1,)), ((), ())), preferred_element_type=jnp.float32)


def kernel(dims, len_ref, x_ref, k_ref, v_ref, wq_ref, wk_ref, wv_ref, wo_ref, cos_ref, sin_ref, y_ref, ko_ref, vo_ref,
           xbuf, raw_k, raw_v, lens, kb, vt, kn, vtn, wbuf, wo1, cosb, sinb, qbuf, ob, pb, oall, ost, kvx, kvr, ybuf, s_scr, sn_scr, acc,
           loc_sem, wq_sem, pair_s, pair_r, q_s, q_r, p_s, p_r, o_s, o_r):
    heads, head_dim, group, tok, cache, cp_size = dims
    my_heads = heads // 2
    half_cols = my_heads * head_dim
    toks = 2 * tok
    pair = 2 * head_dim
    score_c = math.log2(math.e) / math.sqrt(head_dim)

    me = lax.axis_index('cp')
    core = lax.rem(me, 2)
    chip = lax.div(me, 2)
    mate = me + 1 - 2 * core
    peer = lax.rem(me + 2, cp_size)

    def remote(src, dst, send, recv, dev):
        return pltpu.make_async_remote_copy(src_ref=src, dst_ref=dst, send_sem=send, recv_sem=recv, device_id={'cp': dev}, device_id_type=MESH)

    ld_x = pltpu.make_async_copy(x_ref, xbuf.at[pl.ds(pl.multiple_of(core * tok, tok), tok)], loc_sem.at[0])
    ld_cos = pltpu.make_async_copy(cos_ref.at[chip], cosb, loc_sem.at[1])
    ld_sin = pltpu.make_async_copy(sin_ref.at[chip], sinb, loc_sem.at[2])
    ld_k = pltpu.make_async_copy(k_ref.at[:, core], raw_k.at[0], loc_sem.at[3])
    ld_v = pltpu.make_async_copy(v_ref.at[:, core], raw_v.at[0], loc_sem.at[4])
    n_chunk = my_heads // 2

    def ld_wq(j, sem=None):
        sem = j if sem is None else sem
        col = pl.multiple_of(core * half_cols + j * pair, pair)
        return pltpu.make_async_copy(wq_ref.at[:, pl.ds(col, pair)], wbuf.at[:, pl.ds(pl.multiple_of(j * pair, pair), pair)], wq_sem.at[sem])

    kv_col = pl.multiple_of(core * pair, pair)
    ld_wk = pltpu.make_async_copy(wk_ref.at[:, pl.ds(kv_col, pair)], wbuf.at[:, pl.ds(half_cols, pair)], wq_sem.at[n_chunk])
    ld_wv = pltpu.make_async_copy(wv_ref.at[:, pl.ds(kv_col, pair)], wbuf.at[:, pl.ds(half_cols + pair, pair)], wq_sem.at[n_chunk + 1])
    wide = wbuf.shape[1]
    rest = wo1.shape[1]
    ld_wo0 = pltpu.make_async_copy(wo_ref.at[:, pl.ds(0, wide)], wbuf, loc_sem.at[7])
    ld_wo1 = pltpu.make_async_copy(wo_ref.at[:, pl.ds(wide, rest)], wo1, loc_sem.at[8])
    ld_x.start()
    ld_cos.start()
    ld_sin.start()
    ld_k.start()
    ld_v.start()
    lens[0] = jnp.full(lens.shape[1:], len_ref[0], jnp.int32)

    barrier = pltpu.get_barrier_semaphore()
    for other in (mate, peer):
        pl.semaphore_signal(barrier, inc=1, device_id={'cp': other}, device_id_type=MESH)
    pl.semaphore_wait(barrier, 2)

    my_rows = pl.ds(pl.multiple_of(core * tok, tok), tok)
    mate_rows = pl.ds(pl.multiple_of((1 - core) * tok, tok), tok)
    cp_x = remote(x_ref, xbuf.at[my_rows], pair_s.at[0], pair_r.at[0], mate)
    cp_len = remote(lens.at[0], lens.at[1], pair_s.at[1], pair_r.at[1], mate)
    cp_k = remote(k_ref.at[:, 1 - core], raw_k.at[1], pair_s.at[2], pair_r.at[2], mate)
    cp_v = remote(v_ref.at[:, 1 - core], raw_v.at[1], pair_s.at[3], pair_r.at[3], mate)
    cp_x.start()
    cp_len.start()
    for j in range(2):
        ld_wq(j).start()
    cp_k.start()
    cp_v.start()
    for j in range(2, n_chunk):
        ld_wq(j).start()
    ld_wk.start()
    ld_wv.start()

    row = lax.broadcasted_iota(jnp.int32, (2 * PREP, 2 * PREP), 0)
    col = lax.broadcasted_iota(jnp.int32, (2 * PREP, 2 * PREP), 1)
    want = jnp.where(row < PREP, 2 * row, 2 * (row - PREP) + 1)
    pick = jnp.where(col == want, 1.0, 0.0).astype(jnp.bfloat16)
    want_back = jnp.where(col < PREP, 2 * col, 2 * (col - PREP) + 1)
    weave = jnp.where(row == want_back, 1.0, 0.0).astype(jnp.bfloat16)
    lane = lax.broadcasted_iota(jnp.int32, (PREP, head_dim), 1)
    slot = lax.broadcasted_iota(jnp.int32, (PREP, head_dim), 0)

    def prep(block):
        flat_k = raw_k.at[block].reshape(2 * cache, head_dim)
        flat_v = raw_v.at[block].reshape(2 * cache, head_dim)

        def step(i, carry):
            for g in range(PREP_GROUPS):
                at = pl.multiple_of((i * PREP_GROUPS + g) * PREP, PREP)
                to = pl.multiple_of(block * cache + at, PREP)
                both = jnp.concatenate([flat_k[pl.ds(2 * at, 2 * PREP)], flat_v[pl.ds(2 * at, 2 * PREP)]], axis=1)
                split = jnp.dot(pick, both, preferred_element_type=jnp.float32).astype(jnp.bfloat16)
                hidden = jnp.where((slot + at >= lens[block, 0:1, :]) & (lane == 0), HIDE, 0.0).astype(jnp.bfloat16)
                for h in range(2):
                    part = split[h * PREP:(h + 1) * PREP]
                    kb[h, pl.ds(to, PREP), :head_dim] = part[:, :head_dim]
                    kb[h, pl.ds(to, PREP), head_dim:] = hidden
                    vt[h, :, pl.ds(to, PREP)] = part[:, head_dim:].T
            return carry

        lax.fori_loop(0, cache // PREP // PREP_GROUPS, step, 0)

    ld_k.wait()
    ld_v.wait()
    prep(0)

    def rope(vals):
        return vals * cosb[...] + pltpu.roll(vals, head_dim // 2, 1) * sinb[...]

    def cp_q(j):
        src = qbuf.at[pl.ds(2 * j, 2)]
        return remote(src, qbuf.at[pl.ds(my_heads + 2 * j, 2)], q_s.at[j], q_r.at[j], peer)

    ld_x.wait()
    ld_cos.wait()
    ld_sin.wait()
    cp_x.wait_recv()

    def project(first, count):
        return jnp.dot(xbuf[...], wbuf[:, pl.ds(pl.multiple_of(first * pair, pair), count * pair)], preferred_element_type=jnp.float32)

    def rotate(chunk, count):
        for j in range(count):
            for h in range(2):
                part = s_scr[chunk % 2, j * toks:(j + 1) * toks, h * head_dim:(h + 1) * head_dim]
                qbuf[4 * chunk + 2 * j + h] = rope(part).T.astype(jnp.bfloat16)

    def proj_step(c, carry):
        for j in (2 * c, 2 * c + 1):
            ld_wq(jnp.minimum(j, n_chunk - 1), j).wait()
        proj = project(2 * c, 2)
        rotate(jnp.maximum(c - 1, 0), 2)
        for n in range(2):
            s_scr[c % 2, n * toks:(n + 1) * toks] = proj[:, n * pair:(n + 1) * pair]

        @pl.when(c >= 1)
        def _():
            cp_q(2 * c - 2).start()
            cp_q(2 * c - 1).start()

        return carry

    n_proj = (n_chunk + 1) // 2
    lax.fori_loop(0, n_proj, proj_step, 0)
    last = n_proj - 1
    ld_wv.wait()
    v_proj = project(n_chunk + 1, 1)
    rotate(last, 1)
    cp_q(n_chunk - 1).start()
    ld_wo0.start()
    ld_wo1.start()
    k_heads = [rope(s_scr[last % 2, toks:2 * toks, h * head_dim:(h + 1) * head_dim]).astype(jnp.bfloat16) for h in range(2)]
    v_heads = [v_proj[:, h * head_dim:(h + 1) * head_dim].astype(jnp.bfloat16) for h in range(2)]
    for h in range(2):
        kn[h] = k_heads[h]
        vtn[h] = v_heads[h].T
    for part in range(2):
        rows = slice(part * tok, (part + 1) * tok)
        both = jnp.concatenate([jnp.concatenate([k_heads[h][rows], v_heads[h][rows]], axis=1) for h in range(2)], axis=0)
        mixed = jnp.dot(weave, both, preferred_element_type=jnp.float32).astype(jnp.bfloat16)
        for n in range(2):
            kvx[n, rows] = mixed[:, n * head_dim:(n + 1) * head_dim].reshape(tok, 2, head_dim)
    cp_ko = remote(kvx.at[0, mate_rows], kvr.at[0], pair_s.at[4], pair_r.at[4], mate)
    cp_vo = remote(kvx.at[1, mate_rows], kvr.at[1], pair_s.at[5], pair_r.at[5], mate)
    cp_ko.start()
    cp_vo.start()
    outs = [pltpu.make_async_copy(kvx.at[n, my_rows], out_ref.at[:, core], loc_sem.at[9 + n]) for n, out_ref in ((0, ko_ref), (1, vo_ref))]
    for out in outs:
        out.start()

    cp_len.wait_recv()
    cp_k.wait_recv()
    cp_v.wait_recv()
    prep(1)

    n_tiles = 2 * cache // KEY_TILE
    n_sub = KEY_TILE // SUB
    first_a = 2
    new_at = 3
    ones_row = jnp.where(lax.broadcasted_iota(jnp.int32, (head_dim, toks), 0) == 0, 1.0, 0.0).astype(jnp.bfloat16)

    def positions(chip_id, axis):
        within = lax.broadcasted_iota(jnp.int32, (toks, toks), axis)
        dev = 2 * chip_id + jnp.where(within >= tok, 1, 0)
        inner = jnp.where(within >= tok, within - tok, within)
        late = inner >= tok // 2
        piece_id = jnp.where(late, 2 * cp_size - 1 - dev, dev)
        return piece_id * (tok // 2) + jnp.where(late, inner - tok // 2, inner)

    def cp_p(h):
        return remote(ob.at[my_heads + h], pb.at[h], p_s.at[h], p_r.at[h], peer)

    def place(i):
        is_b = jnp.logical_and(i >= first_a, i < first_a + group)
        j = jnp.where(i < first_a, i, jnp.where(is_b, i - first_a, i - group))
        return is_b, jnp.where(is_b, my_heads + j, j), j

    def peak(s):
        return jnp.max(s.reshape(s.shape[0] // 8, 8, toks), axis=0)

    def scores(kvh, q_aug, t, r):
        s = jnp.dot(kb[kvh, t * KEY_TILE + r * SUB:t * KEY_TILE + (r + 1) * SUB], q_aug, preferred_element_type=jnp.float32)
        s_scr[t % 2, r * SUB:(r + 1) * SUB] = s
        return peak(s)

    def with_ones(q):
        return jnp.concatenate([q, ones_row], axis=0)

    def one_head(kvh, idx, next_kvh, next_idx, tops, q_chip):
        q_aug = with_ones(qbuf[idx])
        next_q = with_ones(qbuf[next_idx])
        tops = list(tops)
        top = None
        total = None
        for t in range(n_tiles):
            here = tops[t]
            if t == new_at:
                here = jnp.maximum(here, seg_tops)
            tile_top = jnp.max(here, axis=0, keepdims=True)
            new_top = tile_top if top is None else jnp.maximum(top, tile_top)
            keep = None if top is None else jnp.exp2((top - new_top) * score_c)
            top = new_top
            new_tops = None
            w_sum = None
            halves = []
            for r in range(n_sub):
                w = jnp.exp2((s_scr[t % 2, r * SUB:(r + 1) * SUB] - top) * score_c)
                if t + 2 < n_tiles:
                    sub_tops = scores(kvh, q_aug, t + 2, r)
                else:
                    sub_tops = scores(next_kvh, next_q, t + 2 - n_tiles, r)
                new_tops = sub_tops if new_tops is None else jnp.maximum(new_tops, sub_tops)
                part = jnp.sum(w.reshape(SUB // 8, 8, toks), axis=0)
                w_sum = part if w_sum is None else w_sum + part
                halves.append(w.astype(jnp.bfloat16))
                if len(halves) == PV_SUBS:
                    at = t * KEY_TILE + (r + 1 - PV_SUBS) * SUB
                    wide = halves[0] if PV_SUBS == 1 else jnp.concatenate(halves, axis=0)
                    halves = []
                    out = jnp.dot(vt[kvh, :, at:at + PV_SUBS * SUB], wide, preferred_element_type=jnp.float32)
                    if r + 1 > PV_SUBS:
                        acc[...] += out
                    elif keep is None:
                        acc[...] = out
                    else:
                        acc[...] = acc[...] * keep + out
            if t == new_at - 2:
                s = jnp.dot(kn[kvh], qbuf[idx], preferred_element_type=jnp.float32)
                s = jnp.where(positions(chip, 0) <= positions(q_chip, 1), s, -jnp.inf)
                sn_scr[...] = s
                seg_tops = peak(s)
            if t == new_at:
                w = jnp.exp2((sn_scr[...] - top) * score_c)
                w_sum = w_sum + jnp.sum(w.reshape(toks // 8, 8, toks), axis=0)
                acc[...] += jnp.dot(vtn[kvh], w.astype(jnp.bfloat16), preferred_element_type=jnp.float32)
            total = w_sum if keep is None else total * keep + w_sum
            tops.append(new_tops)
        ob[idx, :head_dim] = acc[...]
        ob[idx, head_dim:head_dim + 8] = jnp.broadcast_to(top, (8, toks))
        ob[idx, head_dim + 8:head_dim + 16] = jnp.broadcast_to(jnp.sum(total, axis=0, keepdims=True), (8, toks))

        return tops[n_tiles], tops[n_tiles + 1]

    def attend(i, tops):
        is_b, idx, j = place(i)
        q_chip = jnp.where(is_b, 1 - chip, chip)
        after = jnp.minimum(i + 1, 2 * group - 1)
        next_b, next_idx, next_j = place(after)
        fresh = jnp.logical_and(next_b, after > i)
        odd = lax.rem(next_j, 2) == 1

        @pl.when(jnp.logical_and(fresh, jnp.logical_and(jnp.logical_not(odd), next_j < group - 1)))
        def _():
            cp_q(lax.div(next_j, 2)).wait_recv()

        @pl.when(jnp.logical_and(fresh, odd))
        def _():
            cp_q(lax.div(next_j + group, 2)).wait_recv()

        @pl.when(jnp.logical_and(fresh, next_j == 0))
        def _():
            cp_q(group // 2).wait_recv()

        tops = one_head(0, idx, 1, idx + group, tops, q_chip)
        tops = one_head(1, idx + group, 0, next_idx, tops, q_chip)

        @pl.when(is_b)
        def _():
            cp_p(j).start()
            cp_p(j + group).start()

        return tops

    first_q = with_ones(qbuf[0])
    start_tops = []
    for t in range(2):
        tops = scores(0, first_q, t, 0)
        for r in range(1, n_sub):
            tops = jnp.maximum(tops, scores(0, first_q, t, r))
        start_tops.append(tops)
    lax.fori_loop(0, 2 * group, attend, tuple(start_tops))

    cp_ko.wait()
    cp_vo.wait()
    more = [pltpu.make_async_copy(kvr.at[n], out_ref.at[:, 1 - core], loc_sem.at[11 + n]) for n, out_ref in ((0, ko_ref), (1, vo_ref))]
    for out in more:
        out.start()

    def cp_o(h):
        col = pl.multiple_of((core * my_heads + h) * head_dim, head_dim)
        return remote(ost.at[h, mate_rows], oall.at[:, pl.ds(col, head_dim)], o_s.at[h], o_r.at[h], mate)

    def combine_one(h):
        top_a, top_b = ob[h, head_dim:head_dim + 1], pb[h, head_dim:head_dim + 1]
        top = jnp.maximum(top_a, top_b)
        keep_a = jnp.exp2((top_a - top) * score_c)
        keep_b = jnp.exp2((top_b - top) * score_c)
        total = ob[h, head_dim + 8:head_dim + 9] * keep_a + pb[h, head_dim + 8:head_dim + 9] * keep_b
        out = (ob[h, :head_dim] * keep_a + pb[h, :head_dim] * keep_b) / total
        ost[h] = out.T.astype(jnp.bfloat16)
        col = pl.multiple_of((core * my_heads + h) * head_dim, head_dim)
        oall[:, pl.ds(col, head_dim)] = ost[h, my_rows]

    def combine(j, carry):
        for h in range(group):
            cp_p(j * group + h).wait_recv()
        for h in range(group):
            combine_one(j * group + h)
        for h in range(group):
            cp_o(j * group + h).start()
        return carry

    lax.fori_loop(0, 2, combine, 0)
    ld_wo0.wait()
    ld_wo1.wait()

    own = pl.ds(pl.multiple_of(core * half_cols, half_cols), half_cols)
    other = pl.ds(pl.multiple_of((1 - core) * half_cols, half_cols), half_cols)
    spans = [(wbuf, n * pair, n * pair) for n in range(wide // pair)] + [(wo1, n * pair, wide + n * pair) for n in range(rest // pair)]

    def y_part(weights, at, rows):
        return jnp.dot(oall[:, rows], weights[rows, at:at + pair], preferred_element_type=jnp.float32)

    for n, (weights, at, _) in enumerate(spans):
        s_scr[n // 8, (n % 8) * tok:(n % 8 + 1) * tok] = y_part(weights, at, own)

    def drain(h, carry):
        cp_o(h).wait()
        cp_p(h).wait_send()
        return carry

    lax.fori_loop(0, my_heads, drain, 0)
    y_copies = []
    cuts = [len(spans) // 2, len(spans)]
    for n, (weights, at, col) in enumerate(spans):
        part = s_scr[n // 8, (n % 8) * tok:(n % 8 + 1) * tok] + y_part(weights, at, other)
        ybuf[:, col:col + pair] = part.astype(jnp.bfloat16)
        if n + 1 in cuts:
            which = cuts.index(n + 1)
            first = 0 if which == 0 else spans[cuts[which - 1]][2]
            cols = pl.ds(first, col + pair - first)
            y_copies.append(pltpu.make_async_copy(ybuf.at[:, cols], y_ref.at[:, cols], loc_sem.at[13 + which]))
            y_copies[-1].start()
    for out in y_copies + outs + more:
        out.wait()
    for j in range(n_chunk):
        cp_q(j).wait_send()
    for copy in (cp_x, cp_len, cp_k, cp_v):
        copy.wait_send()


def hand_on(y_in, k_in, v_in, y_ref, k_ref, v_ref, y_buf, k_buf, v_buf, in_sem, out_sem):
    rows = y_in.shape[0] // 4
    parts = [(src.at[...], buf.at[...], dst.at[...]) for src, buf, dst in ((k_in, k_buf, k_ref), (v_in, v_buf, v_ref))]
    for n in range(4):
        cut = pl.ds(n * rows, rows)
        parts.append((y_in.at[cut], y_buf.at[cut], y_ref.at[cut]))
    loads = [pltpu.make_async_copy(src, buf, in_sem.at[n]) for n, (src, buf, _) in enumerate(parts)]
    stores = [pltpu.make_async_copy(buf, dst, out_sem.at[n]) for n, (_, buf, dst) in enumerate(parts)]
    for load in loads:
        load.start()
    for load, store in zip(loads, stores):
        load.wait()
        store.start()
    for store in stores:
        store.wait()


def solution(mesh):
    cp_size = mesh.shape['cp']
    row_spec = P(('dp', 'cp'), None)
    cache_spec = P(('dp', 'cp'), None, None)
    len_spec = P(('dp', 'cp'))
    full_spec = P()

    def device_fn(x_new, k_cache, v_cache, valid_len, w_q, w_k, w_v, w_o):
        tok, width = x_new.shape
        cache, kv_heads, head_dim = k_cache.shape
        heads = w_q.shape[1] // head_dim
        my_heads = heads // 2
        toks = 2 * tok
        half_cols = my_heads * head_dim
        cos, sin = rope_constants(tok, cp_size, cache * cp_size, head_dim)
        dims = (heads, head_dim, heads // kv_heads, tok, cache, cp_size)
        bf16, f32 = jnp.bfloat16, jnp.float32
        k4 = k_cache.reshape(cache, 2, 2, head_dim)
        v4 = v_cache.reshape(cache, 2, 2, head_dim)
        any_spec = pl.BlockSpec(memory_space=pl.ANY)
        dma = pltpu.SemaphoreType.DMA
        y_out, k_new, v_new = pl.pallas_call(
            functools.partial(kernel, dims),
            out_shape=(
                jax.ShapeDtypeStruct((tok, width), bf16),
                jax.ShapeDtypeStruct((tok, kv_heads // 2, 2, head_dim), bf16),
                jax.ShapeDtypeStruct((tok, kv_heads // 2, 2, head_dim), bf16),
            ),
            in_specs=[pl.BlockSpec(memory_space=pltpu.SMEM)] + [any_spec] * 9,
            out_specs=(any_spec,) * 3,
            scratch_shapes=[
                pltpu.VMEM((toks, width), bf16),
                pltpu.VMEM((2, cache, 2, head_dim), bf16),
                pltpu.VMEM((2, cache, 2, head_dim), bf16),
                pltpu.VMEM((2, 8, head_dim), jnp.int32),
                pltpu.VMEM((2, 2 * cache, 2 * head_dim), bf16),
                pltpu.VMEM((2, head_dim, 2 * cache), bf16),
                pltpu.VMEM((2, toks, head_dim), bf16),
                pltpu.VMEM((2, head_dim, toks), bf16),
                pltpu.VMEM((width, half_cols + 4 * head_dim), bf16),
                pltpu.VMEM((width, heads * head_dim - half_cols - 4 * head_dim), bf16),
                pltpu.VMEM((toks, head_dim), f32),
                pltpu.VMEM((toks, head_dim), f32),
                pltpu.VMEM((heads, head_dim, toks), bf16),
                pltpu.VMEM((heads, head_dim + 16, toks), f32),
                pltpu.VMEM((my_heads, head_dim + 16, toks), f32),
                pltpu.VMEM((tok, heads * head_dim), bf16),
                pltpu.VMEM((my_heads, toks, head_dim), bf16),
                pltpu.VMEM((2, toks, 2, head_dim), bf16),
                pltpu.VMEM((2, tok, 2, head_dim), bf16),
                pltpu.VMEM((tok, width), bf16),
                pltpu.VMEM((2, KEY_TILE, toks), f32),
                pltpu.VMEM((toks, toks), f32),
                pltpu.VMEM((head_dim, toks), f32),
                dma((15,)), dma((my_heads // 2 + 2,)), dma((6,)), dma((6,)),
                dma((my_heads // 2,)), dma((my_heads // 2,)),
                dma((my_heads,)), dma((my_heads,)), dma((my_heads,)), dma((my_heads,)),
            ],
            compiler_params=pltpu.CompilerParams(collective_id=0, has_side_effects=True, vmem_limit_bytes=67043328),
        )(valid_len, x_new, k4, v4, w_q, w_k, w_v, w_o, jnp.asarray(cos), jnp.asarray(sin))
        y_out, k_new, v_new = pl.pallas_call(
            hand_on,
            out_shape=tuple(jax.ShapeDtypeStruct(part.shape, bf16) for part in (y_out, k_new, v_new)),
            in_specs=[any_spec] * 3,
            out_specs=(any_spec,) * 3,
            scratch_shapes=[pltpu.VMEM(part.shape, bf16) for part in (y_out, k_new, v_new)] + [dma((6,)), dma((6,))],
        )(y_out, k_new, v_new)
        shape = (tok, kv_heads, head_dim)
        return y_out, k_new.reshape(shape), v_new.reshape(shape)

    return jax.shard_map(device_fn, mesh=mesh, in_specs=(row_spec, cache_spec, cache_spec, len_spec, full_spec, full_spec, full_spec, full_spec), out_specs=(row_spec, cache_spec, cache_spec), check_vma=False)
```
